256 devices in a mesh: gx: 4 (over x), gy: 8 (over z_lo, core), gz: 8 (over y, z_hi).
Axes of the slice: x: 4, y: 4, z: 8 (z_hi: 2, z_lo: 4; z = z_hi * 4 + z_lo), core: 2. Of those that a mesh axis runs over, the one named last changes fastest.
Arguments:
- energy: float32 [256, 256, 1024], P(('gz', 'gy', 'gx')), may hold values from -5 to 5
- flow: float32 [4, 256, 256, 1024], P(None, ('gz', 'gy', 'gx')), may hold values from -0.1 to 0.12, as said below
Outputs:
- energy_next: float32 [256, 256, 1024], P('gz', 'gx', 'gy')
- plane_mean: float32 [256], P('gz')
- running_mean: float32 [256], P('gz')
The draws below stay inside these ranges and needn't reach their ends.
Inputs may be any that keep to these rules, and one draw needn't show every extreme that they name: flow[0], flow[1] and flow[2] lie within -0.1 to 0.1; flow[3] lies within 0.02 to 0.12.
All inputs are finite; a program needn't handle non-finite values.
Results may differ from the reference program's by a relative error of at most 0.00002.
Values sent between devices are 32-bit elements; how exact they have to be, the bound alone decides.
A program may use at most 128 MiB of HBM per device.

```python
import math
import jax
import jax.numpy as jnp

NX = 256
NY = 1024
NZ = 256


def draw_energy(key, part):
    noise_key, phase_key, offset_key = jax.random.split(jax.random.fold_in(key, 11), 3)
    phases = jax.random.uniform(phase_key, (3,), jnp.float32, 0.0, 2.0 * math.pi)
    z_fraction = (jnp.arange(NZ, dtype=jnp.float32) / NZ)[:, None, None]
    x_fraction = (jnp.arange(NX, dtype=jnp.float32) / NX)[None, :, None]
    y_fraction = (jnp.arange(NY, dtype=jnp.float32) / NY)[None, None, :]
    offsets = jax.random.uniform(offset_key, (NZ, 1, 1), jnp.float32, -1.2, 1.2)
    smooth = offsets + 0.6 * jnp.sin(2.0 * math.pi * x_fraction + phases[0]) * jnp.cos(2.0 * math.pi * z_fraction + phases[1]) + 0.3 * jnp.cos(2.0 * math.pi * y_fraction + phases[2])
    noise = 0.8 * jnp.clip(jax.random.normal(noise_key, (NZ, NX, NY), jnp.float32), -3.0, 3.0)
    return (smooth + noise).astype(jnp.float32)


def draw_flow(key, part):
    speed_key, kappa_key = jax.random.split(jax.random.fold_in(key, 23))
    speeds = jax.random.uniform(speed_key, (3, NZ, NX, NY), jnp.float32, -0.1, 0.1)
    conductivity = jnp.exp(jax.random.uniform(kappa_key, (1, NZ, NX, NY), jnp.float32, math.log(0.02), math.log(0.12)))
    return jnp.concatenate([speeds, conductivity], 0).astype(jnp.float32)


def setup_inputs(seed: int = 0) -> dict:
    seeds = jax.random.split(jax.random.key(seed), 3)
    return {
        "energy": draw_energy(jax.random.fold_in(seeds[2], 71), 0),
        "flow": draw_flow(jax.random.fold_in(seeds[2], 71), 0),
    }


directions = ((1, 0, 0), (0, 1, 0), (0, 0, 1))


def extend(field):
    padded = jnp.pad(field, ((0, 0), (1, 1), (1, 1)))
    return jnp.concatenate([padded[-1:], padded, padded[:1]], 0)


def window(array, offset):
    return array[1 + offset[0]: array.shape[0] - 1 + offset[0],
                 1 + offset[1]: array.shape[1] - 1 + offset[1],
                 1 + offset[2]: array.shape[2] - 1 + offset[2]]


def advance(energy_pad, kappa_pad, velocity):
    centre = window(energy_pad, (0, 0, 0))
    kappa_centre = window(kappa_pad, (0, 0, 0))
    change = jnp.zeros_like(centre)
    for axis_number, forward in enumerate(directions):
        backward = tuple(-item for item in forward)
        upper = window(energy_pad, forward)
        lower = window(energy_pad, backward)
        kappa_upper = window(kappa_pad, forward)
        kappa_lower = window(kappa_pad, backward)
        change = change + 0.5 * (kappa_centre + kappa_upper) * (upper - centre) - 0.5 * (kappa_centre + kappa_lower) * (centre - lower)
        speed = velocity[axis_number]
        change = change - jnp.maximum(speed, 0.0) * (centre - lower) - jnp.minimum(speed, 0.0) * (upper - centre)
    return centre + change


def reference(energy, flow):
    velocity = flow[:3]
    kappa_pad = extend(flow[3])
    energy_half = advance(extend(energy), kappa_pad, velocity)
    energy_next = advance(extend(energy_half), kappa_pad, velocity)
    plane_mean = jnp.sum(energy_next, axis=(1, 2)) / (NX * NY)
    ranks = jnp.arange(1, NZ + 1).astype(jnp.float32)
    running_mean = jnp.cumsum(plane_mean) / ranks
    return energy_next, plane_mean, running_mean
```

```python
import functools

import jax
import jax.numpy as jnp
from jax import lax
from jax.experimental import pallas as pl
from jax.experimental.pallas import tpu as pltpu
from jax.sharding import PartitionSpec as P

MESH = pl.DeviceIdType.MESH
AHEAD = 3


def change_of(X, p, xi, F, fi):
    here = X[p, :, pl.ds(xi, 8), :]
    kappa = F[3, p, :, pl.ds(fi, 8), :]
    lane = lax.broadcasted_iota(jnp.int32, here.shape, 2)
    none = jnp.zeros_like(here[:1])

    def right(v):
        r = pltpu.roll(v, 127, 2)
        return jnp.where(lane == 127, jnp.concatenate([r[1:], none], 0), r)

    def left(v):
        r = pltpu.roll(v, 1, 2)
        return jnp.where(lane == 0, jnp.concatenate([none, r[:-1]], 0), r)

    sides = (
        (
            0,
            X[p + 1, :, pl.ds(xi, 8), :],
            F[3, p + 1, :, pl.ds(fi, 8), :],
            X[p - 1, :, pl.ds(xi, 8), :],
            F[3, p - 1, :, pl.ds(fi, 8), :],
        ),
        (
            1,
            X[p, :, pl.ds(xi + 1, 8), :],
            F[3, p, :, pl.ds(fi + 1, 8), :],
            X[p, :, pl.ds(xi - 1, 8), :],
            F[3, p, :, pl.ds(fi - 1, 8), :],
        ),
        (2, right(here), right(kappa), left(here), left(kappa)),
    )
    change = jnp.zeros_like(here)
    for axis, upper, kappa_upper, lower, kappa_lower in sides:
        speed = F[axis, p, :, pl.ds(fi, 8), :]
        change = (
            change
            + (0.5 * (kappa + kappa_upper) - jnp.minimum(speed, 0.0)) * (upper - here)
            - (0.5 * (kappa + kappa_lower) + jnp.maximum(speed, 0.0)) * (here - lower)
        )
    return here + change


def kernel(
    nx, ny, nz, e_ref, f_ref, o_ref, pm_ref, rm_ref, E, F, H, N, acc, SA, SB, SC, SM,
    xsE, xsF, xrE, xrF, gsE, gsK, gsU, grE, grK, grU, zsE, zsK, zsH, zrE, zrK, zrH,
    osem, orem, sa_s, sa_r, sb_s, sb_r, sc_s, sc_r, tok,
):
    gx, gy, gz = (lax.axis_index(a) for a in ("gx", "gy", "gz"))
    ring = ny * nz
    m = gz * ny + gy
    up, down = lax.rem(m + 1, ring), lax.rem(m + ring - 1, ring)
    chain = tuple({"gy": lax.rem(n, ny), "gz": n // ny} for n in (up, down))
    rows = 64
    tiles = rows // 8

    bar = pltpu.get_barrier_semaphore()
    for d in range(1, nx):
        pl.semaphore_signal(
            bar, inc=1, device_id={"gx": lax.rem(gx + d, nx)}, device_id_type=MESH
        )
    for to in chain:
        pl.semaphore_signal(bar, inc=1, device_id=to, device_id_type=MESH)

    def copy(src, dst, send, recv, to):
        return pltpu.make_async_remote_copy(
            src_ref=src, dst_ref=dst, send_sem=send, recv_sem=recv, device_id=to,
            device_id_type=MESH,
        )

    def x_tile(d, c):
        t = lax.rem(gx + d, nx)
        src = (e_ref.at[t * tiles + c], f_ref.at[:, t * tiles + c])
        at = pl.ds(pl.multiple_of(8 + 8 * c, 8), 8)
        dst = (E.at[1 + gx, :, at, :], F.at[:, 1 + gx, :, at, :])
        if d == 0:
            return (
                pltpu.make_async_copy(src[0], dst[0], xrE.at[0, c]),
                pltpu.make_async_copy(src[1], dst[1], xrF.at[0, c]),
            )
        return (
            copy(src[0], dst[0], xsE.at[d], xrE.at[d, c], {"gx": t}),
            copy(src[1], dst[1], xsF.at[d], xrF.at[d, c], {"gx": t}),
        )

    def x_edge(d, side):
        t = lax.rem(gx + d, nx)
        if side == 0:
            tile = lax.max(t * tiles - 1, 0)
            wide, narrow, wide_at, narrow_at = pl.ds(6, 2), pl.ds(7, 1), pl.ds(6, 2), pl.ds(7, 1)
        else:
            tile = lax.min((t + 1) * tiles, nx * tiles - 1)
            wide, narrow = pl.ds(0, 2), pl.ds(0, 1)
            wide_at, narrow_at = pl.ds(8 + rows, 2), pl.ds(8 + rows, 1)
        parts = (
            (e_ref.at[tile, :, wide, :], E.at[1 + gx, :, wide_at, :], gsE, grE),
            (f_ref.at[3, tile, :, wide, :], F.at[3, 1 + gx, :, wide_at, :], gsK, grK),
            (
                f_ref.at[pl.ds(0, 3), tile, :, narrow, :],
                F.at[pl.ds(0, 3), 1 + gx, :, narrow_at, :],
                gsU,
                grU,
            ),
        )
        if d == 0:
            return [pltpu.make_async_copy(a, b, r.at[0, side]) for a, b, s, r in parts]
        return [copy(a, b, s.at[d, side], r.at[d, side], {"gx": t}) for a, b, s, r in parts]

    def has_edge(g, side):
        return g > 0 if side == 0 else g < nx - 1

    def start_tile(c):
        for d in (0, *range(1, nx)):
            for x in x_tile(d, c):
                x.start()

    def start_edges(side):
        for d in range(nx):

            @pl.when(has_edge(lax.rem(gx + d, nx), side))
            def _():
                for x in x_edge(d, side):
                    x.start()

    def z_window(way, at, c):
        src, dst = ((4, 0), (1, 5))[way]
        return (
            copy(E.at[src, :, at, :], E.at[dst, :, at, :], zsE.at[way], zrE.at[way, c], chain[way]),
            copy(
                F.at[3, src, :, at, :], F.at[3, dst, :, at, :], zsK.at[way], zrK.at[way, c],
                chain[way],
            ),
        )

    def h_window(way, at, c):
        src, dst = ((4, 0), (1, 5))[way]
        return copy(
            H.at[src, :, at, :], H.at[dst, :, at, :], zsH.at[way], zrH.at[way, c], chain[way]
        )

    def out_window(d, src_at, dst_at):
        t = lax.rem(gy + d, ny)
        return copy(
            N.at[:, t, src_at, :], o_ref.at[pl.ds(4 * gy, 4), dst_at, :], osem.at[d], orem.at[d],
            {"gy": t},
        )

    def send_out(src_at, dst_at):
        def one(d, _):
            out_window(d, src_at, dst_at).start()
            return 0

        lax.fori_loop(1, ny, one, 0)
        pltpu.make_async_copy(
            N.at[:, gy, src_at, :], o_ref.at[pl.ds(4 * gy, 4), dst_at, :], orem.at[0]
        ).start()

    def half(c):
        def plane(p, _):
            v = change_of(E, p, 8 * c + 7, F, 8 * c + 7)
            r = lax.broadcasted_iota(jnp.int32, v.shape, 1) + (8 * c - 1 + rows * gx)
            H[p, :, pl.ds(pl.multiple_of(8 * c + 8, 8), 8), :] = jnp.where(
                (r >= 0) & (r < rows * nx), v, 0.0
            )
            return 0

        lax.fori_loop(1, 5, plane, 0)

    def full(c):
        def plane(p, _):
            v = change_of(H, p, 8 * c + 7, F, 8 * c + 6)
            N[p - 1, :, pl.ds(pl.multiple_of(8 * c, 8), 8), :] = v
            r = lax.broadcasted_iota(jnp.int32, v.shape, 1) + (8 * c - 2)
            acc[p - 1] += jnp.sum(jnp.where((r >= 0) & (r < rows), v, 0.0), axis=0)
            return 0

        lax.fori_loop(1, 5, plane, 0)

    def wait_tile(c):
        for d in range(nx):
            for x in x_tile(d, c):
                x.wait() if d == 0 else x.wait_recv()

    def wait_edges(side):
        @pl.when(has_edge(gx, side))
        def _():
            for d in range(nx):
                for x in x_edge(d, side):
                    x.wait() if d == 0 else x.wait_recv()

    def body_at(c):
        return pl.ds(pl.multiple_of(8 * c, 8), 8), pl.ds(8 * c - 2, 8)

    first_at = (pl.ds(2, 6), pl.ds(0, 6))

    acc[...] = jnp.zeros_like(acc)
    for side, at in ((0, slice(6, 8)), (1, slice(8 + rows, 10 + rows))):

        @pl.when(jnp.logical_not(has_edge(gx, side)))
        def _():
            E[1:5, :, at, :] = jnp.zeros_like(E[1:5, :, at, :])
            F[3, 1:5, :, at, :] = jnp.zeros_like(E[1:5, :, at, :])

    pl.semaphore_wait(bar, nx + 1)
    start_edges(0)
    start_tile(0)
    start_edges(1)
    for c in range(1, AHEAD):
        start_tile(c)
    wait_edges(0)

    def step(c, _):
        @pl.when(c + AHEAD < tiles)
        def _():
            start_tile(c + AHEAD)

        wait_tile(c)
        at = pl.ds(8 * c + 7, 8)
        for way in (0, 1):
            for x in z_window(way, at, c):
                x.start()
        for way in (0, 1):
            for x in z_window(way, at, c):
                x.wait_recv()
        half(c)
        at = pl.ds(pl.multiple_of(8 * c + 8, 8), 8)
        for way in (0, 1):
            h_window(way, at, c).start()
        for way in (0, 1):
            h_window(way, at, c).wait_recv()
        full(c)

        @pl.when(c == 2)
        def _():
            send_out(*first_at)
            send_out(*body_at(1))

        @pl.when(c >= 2)
        def _():
            send_out(*body_at(c))

        for at_step, hop, slot in ((4, 1, 0), (5, 2, 1)):

            @pl.when(c == at_step)
            def _():
                for n in (hop, nz - hop):
                    pl.semaphore_signal(
                        tok.at[slot], inc=1, device_id={"gz": lax.rem(gz + n, nz)},
                        device_id_type=MESH,
                    )

            @pl.when(c == at_step + 1)
            def _():
                pl.semaphore_wait(tok.at[slot], 2)

        return 0

    lax.fori_loop(0, tiles - 1, step, 0)

    last = tiles - 1
    wait_edges(1)
    wait_tile(last)
    ends = ((pl.ds(8 * last + 7, 8), last), (pl.ds(8 * tiles + 7, 2), tiles))
    for at, c in ends:
        for way in (0, 1):
            for x in z_window(way, at, c):
                x.start()
    for at, c in ends:
        for way in (0, 1):
            for x in z_window(way, at, c):
                x.wait_recv()
    half(last)
    half(tiles)
    ends = ((pl.ds(8 * last + 8, 8), last), (pl.ds(8 * tiles + 8, 1), tiles))
    for at, c in ends:
        for way in (0, 1):
            h_window(way, at, c).start()
    for at, c in ends:
        for way in (0, 1):
            h_window(way, at, c).wait_recv()
    full(last)
    full(tiles)
    send_out(*body_at(last))
    send_out(pl.ds(8 * tiles, 2), pl.ds(rows - 2, 2))

    def meet(own, box, axis, size, me, send, recv):
        for d in range(1, size):
            copy(own, box.at[me], send.at[d], recv.at[d], {axis: lax.rem(me + d, size)}).start()
        for d in range(1, size):
            copy(own, box.at[me], send.at[d], recv.at[d], {axis: lax.rem(me + d, size)}).wait()

    part = jnp.sum(acc[...], axis=1)
    part = jnp.concatenate([part, jnp.zeros_like(part)], 0)
    SM[0] = part
    SA[gx] = part
    meet(SM.at[0], SA, "gx", nx, gx, sa_s, sa_r)
    part = SA[0]
    for i in range(1, nx):
        part = part + SA[i]
    SM[1] = part
    SB[gy] = part
    meet(SM.at[1], SB, "gy", ny, gy, sb_s, sb_r)
    planes = SB[...]
    total = jnp.sum(planes, axis=0)
    SM[2] = total
    SC[gz] = total
    meet(SM.at[2], SC, "gz", nz, gz, sc_s, sc_r)
    offset = jnp.zeros_like(total)
    for i in range(nz):
        offset = offset + jnp.where(i < gz, SC[i], 0.0)
    cells = 1.0 / (rows * nx * 128 * ny)
    run = jnp.sum(offset, axis=(0, 1), keepdims=True) * cells
    row = lax.broadcasted_iota(jnp.int32, (8, 128), 0)
    for g in range(ny):
        mean = jnp.broadcast_to(jnp.sum(planes[g], axis=1, keepdims=True) * cells, (8, 128))
        pm_ref[g] = mean
        upto = mean + jnp.where(row >= 1, pltpu.roll(mean, 1, 0), 0.0)
        upto = upto + jnp.where(row >= 2, pltpu.roll(upto, 2, 0), 0.0)
        rank = (row + (gz * 4 * ny + 4 * g + 1)).astype(jnp.float32)
        rm_ref[g] = (run + upto) / rank
        run = run + upto[3:4, 0:1]

    for d in range(ny):
        whole = o_ref.at[pl.ds(0, 4)]
        if d == 0:
            pltpu.make_async_copy(N.at[:, 0, pl.ds(0, rows), :], whole, orem.at[0]).wait()
        else:
            end = copy(
                N.at[:, 0, pl.ds(0, rows), :], whole, osem.at[d], orem.at[d],
                {"gy": lax.rem(gy + d, ny)},
            )
            end.wait()
    for d in range(1, nx):
        to = {"gx": lax.rem(gx + d, nx)}
        at = pl.ds(8, rows)
        copy(E.at[1, :, at, :], E.at[1, :, at, :], xsE.at[d], xrE.at[d, 0], to).wait_send()
        copy(F.at[:, 1, :, at, :], F.at[:, 1, :, at, :], xsF.at[d], xrF.at[d, 0], to).wait_send()
        for side in (0, 1):

            @pl.when(has_edge(lax.rem(gx + d, nx), side))
            def _():
                for x in x_edge(d, side):
                    x.wait_send()
    for way in (0, 1):
        for x in z_window(way, pl.ds(7, rows + 2), 0):
            x.wait_send()
        h_window(way, pl.ds(8, rows + 1), 0).wait_send()


def per_device(energy, flow):
    nx, ny, nz = (lax.axis_size(a) for a in ("gx", "gy", "gz"))
    e = energy.reshape(32, 8, 8, 128).transpose(0, 2, 1, 3)
    f = flow.reshape(4, 32, 8, 8, 128).transpose(0, 1, 3, 2, 4)
    vmem = pl.BlockSpec(memory_space=pltpu.VMEM)
    hbm = pl.BlockSpec(memory_space=pl.ANY)
    f32 = jnp.float32
    dma = pltpu.SemaphoreType.DMA
    result, mean, running = pl.pallas_call(
        functools.partial(kernel, nx, ny, nz),
        out_shape=(
            jax.ShapeDtypeStruct((32, 64, 128), f32),
            jax.ShapeDtypeStruct((8, 8, 128), f32),
            jax.ShapeDtypeStruct((8, 8, 128), f32),
        ),
        in_specs=[hbm, hbm],
        out_specs=(hbm, vmem, vmem),
        scratch_shapes=[
            pltpu.VMEM((6, 8, 88, 128), f32),
            pltpu.VMEM((4, 6, 8, 88, 128), f32),
            pltpu.VMEM((6, 8, 88, 128), f32),
            pltpu.VMEM((4, 8, 72, 128), f32),
            pltpu.VMEM((4, 8, 128), f32),
            pltpu.VMEM((4, 8, 128), f32),
            pltpu.VMEM((8, 8, 128), f32),
            pltpu.VMEM((8, 8, 128), f32),
            pltpu.VMEM((3, 8, 128), f32),
            dma((4,)), dma((4,)), dma((4, 8)), dma((4, 8)),
            dma((4, 2)), dma((4, 2)), dma((4, 2)), dma((4, 2)), dma((4, 2)), dma((4, 2)),
            dma((2,)), dma((2,)), dma((2,)), dma((2, 9)), dma((2, 9)), dma((2, 9)),
            dma((8,)), dma((8,)),
            dma((4,)), dma((4,)), dma((8,)), dma((8,)), dma((8,)), dma((8,)),
            pltpu.SemaphoreType.REGULAR((2,)),
        ],
        compiler_params=pltpu.CompilerParams(collective_id=0, has_side_effects=True),
        name="two_steps",
    )(e, f)
    return result, mean[:, :4, 0].reshape(-1), running[:, :4, 0].reshape(-1)


def solution(mesh):
    placed = (P(("gz", "gy", "gx"), None, None), P(None, ("gz", "gy", "gx"), None, None))
    return jax.shard_map(
        per_device,
        mesh=mesh,
        in_specs=placed,
        out_specs=(P("gz", "gx", "gy"), P("gz"), P("gz")),
        check_vma=False,
    )
```

```python
import functools

import jax
import jax.numpy as jnp
from jax import lax
from jax.experimental import pallas as pl
from jax.experimental.pallas import tpu as pltpu
from jax.sharding import PartitionSpec as P

MESH = pl.DeviceIdType.MESH
AHEAD = 3


def change_of(X, p, xi, F, fi):
    here = X[p, :, pl.ds(xi, 8), :]
    kappa = F[3, p, :, pl.ds(fi, 8), :]
    lane = lax.broadcasted_iota(jnp.int32, here.shape, 2)
    none = jnp.zeros_like(here[:1])

    def right(v):
        r = pltpu.roll(v, 127, 2)
        return jnp.where(lane == 127, jnp.concatenate([r[1:], none], 0), r)

    def left(v):
        r = pltpu.roll(v, 1, 2)
        return jnp.where(lane == 0, jnp.concatenate([none, r[:-1]], 0), r)

    sides = (
        (
            0,
            X[p + 1, :, pl.ds(xi, 8), :],
            F[3, p + 1, :, pl.ds(fi, 8), :],
            X[p - 1, :, pl.ds(xi, 8), :],
            F[3, p - 1, :, pl.ds(fi, 8), :],
        ),
        (
            1,
            X[p, :, pl.ds(xi + 1, 8), :],
            F[3, p, :, pl.ds(fi + 1, 8), :],
            X[p, :, pl.ds(xi - 1, 8), :],
            F[3, p, :, pl.ds(fi - 1, 8), :],
        ),
        (2, right(here), right(kappa), left(here), left(kappa)),
    )
    change = jnp.zeros_like(here)
    for axis, upper, kappa_upper, lower, kappa_lower in sides:
        speed = F[axis, p, :, pl.ds(fi, 8), :]
        change = (
            change
            + (0.5 * (kappa + kappa_upper) - jnp.minimum(speed, 0.0)) * (upper - here)
            - (0.5 * (kappa + kappa_lower) + jnp.maximum(speed, 0.0)) * (here - lower)
        )
    return here + change


def kernel(
    nx, ny, nz, e_ref, f_ref, o_ref, pm_ref, rm_ref, E, F, H, N, acc, SA, SB, SC, SM,
    xsE, xsF, xrE, xrF, gsE, gsK, gsU, grE, grK, grU, zsE, zsK, zsH, zrE, zrK, zrH,
    osem, orem, sa_s, sa_r, sb_s, sb_r, sc_s, sc_r, tok,
):
    gx, gy, gz = (lax.axis_index(a) for a in ("gx", "gy", "gz"))
    ring = ny * nz
    m = gz * ny + gy
    up, down = lax.rem(m + 1, ring), lax.rem(m + ring - 1, ring)
    chain = tuple({"gy": lax.rem(n, ny), "gz": n // ny} for n in (up, down))
    rounds = (ring - 1).bit_length() - 1
    rows = 64
    tiles = rows // 8

    bar = pltpu.get_barrier_semaphore()
    for d in range(1, nx):
        pl.semaphore_signal(
            bar, inc=1, device_id={"gx": lax.rem(gx + d, nx)}, device_id_type=MESH
        )
    for to in chain:
        pl.semaphore_signal(bar, inc=1, device_id=to, device_id_type=MESH)

    def copy(src, dst, send, recv, to):
        return pltpu.make_async_remote_copy(
            src_ref=src, dst_ref=dst, send_sem=send, recv_sem=recv, device_id=to,
            device_id_type=MESH,
        )

    def x_tile(d, c):
        t = lax.rem(gx + d, nx)
        src = (e_ref.at[t * tiles + c], f_ref.at[:, t * tiles + c])
        at = pl.ds(pl.multiple_of(8 + 8 * c, 8), 8)
        dst = (E.at[1 + gx, :, at, :], F.at[:, 1 + gx, :, at, :])
        if d == 0:
            return (
                pltpu.make_async_copy(src[0], dst[0], xrE.at[0, c]),
                pltpu.make_async_copy(src[1], dst[1], xrF.at[0, c]),
            )
        return (
            copy(src[0], dst[0], xsE.at[d], xrE.at[d, c], {"gx": t}),
            copy(src[1], dst[1], xsF.at[d], xrF.at[d, c], {"gx": t}),
        )

    def x_edge(d, side):
        t = lax.rem(gx + d, nx)
        if side == 0:
            tile = lax.max(t * tiles - 1, 0)
            wide, narrow, wide_at, narrow_at = pl.ds(6, 2), pl.ds(7, 1), pl.ds(6, 2), pl.ds(7, 1)
        else:
            tile = lax.min((t + 1) * tiles, nx * tiles - 1)
            wide, narrow = pl.ds(0, 2), pl.ds(0, 1)
            wide_at, narrow_at = pl.ds(8 + rows, 2), pl.ds(8 + rows, 1)
        parts = (
            (e_ref.at[tile, :, wide, :], E.at[1 + gx, :, wide_at, :], gsE, grE),
            (f_ref.at[3, tile, :, wide, :], F.at[3, 1 + gx, :, wide_at, :], gsK, grK),
            (
                f_ref.at[pl.ds(0, 3), tile, :, narrow, :],
                F.at[pl.ds(0, 3), 1 + gx, :, narrow_at, :],
                gsU,
                grU,
            ),
        )
        if d == 0:
            return [pltpu.make_async_copy(a, b, r.at[0, side]) for a, b, s, r in parts]
        return [copy(a, b, s.at[d, side], r.at[d, side], {"gx": t}) for a, b, s, r in parts]

    def has_edge(g, side):
        return g > 0 if side == 0 else g < nx - 1

    def start_tile(c):
        for d in (0, *range(1, nx)):
            for x in x_tile(d, c):
                x.start()

    def start_edges(side):
        for d in range(nx):

            @pl.when(has_edge(lax.rem(gx + d, nx), side))
            def _():
                for x in x_edge(d, side):
                    x.start()

    def z_window(way, at, c):
        src, dst = ((4, 0), (1, 5))[way]
        return (
            copy(E.at[src, :, at, :], E.at[dst, :, at, :], zsE.at[way], zrE.at[way, c], chain[way]),
            copy(
                F.at[3, src, :, at, :], F.at[3, dst, :, at, :], zsK.at[way], zrK.at[way, c],
                chain[way],
            ),
        )

    def h_window(way, at, c):
        src, dst = ((4, 0), (1, 5))[way]
        return copy(
            H.at[src, :, at, :], H.at[dst, :, at, :], zsH.at[way], zrH.at[way, c], chain[way]
        )

    def out_window(d, src_at, dst_at):
        t = lax.rem(gy + d, ny)
        return copy(
            N.at[:, t, src_at, :], o_ref.at[pl.ds(4 * gy, 4), dst_at, :], osem.at[d], orem.at[d],
            {"gy": t},
        )

    def send_out(src_at, dst_at):
        def one(d, _):
            out_window(d, src_at, dst_at).start()
            return 0

        lax.fori_loop(1, ny, one, 0)
        pltpu.make_async_copy(
            N.at[:, gy, src_at, :], o_ref.at[pl.ds(4 * gy, 4), dst_at, :], orem.at[0]
        ).start()

    def half(c):
        def plane(p, _):
            v = change_of(E, p, 8 * c + 7, F, 8 * c + 7)
            r = lax.broadcasted_iota(jnp.int32, v.shape, 1) + (8 * c - 1 + rows * gx)
            H[p, :, pl.ds(pl.multiple_of(8 * c + 8, 8), 8), :] = jnp.where(
                (r >= 0) & (r < rows * nx), v, 0.0
            )
            return 0

        lax.fori_loop(1, 5, plane, 0)

    def full(c):
        def plane(p, _):
            v = change_of(H, p, 8 * c + 7, F, 8 * c + 6)
            N[p - 1, :, pl.ds(pl.multiple_of(8 * c, 8), 8), :] = v
            r = lax.broadcasted_iota(jnp.int32, v.shape, 1) + (8 * c - 2)
            acc[p - 1] += jnp.sum(jnp.where((r >= 0) & (r < rows), v, 0.0), axis=0)
            return 0

        lax.fori_loop(1, 5, plane, 0)

    def wait_tile(c):
        for d in range(nx):
            for x in x_tile(d, c):
                x.wait() if d == 0 else x.wait_recv()

    def wait_edges(side):
        @pl.when(has_edge(gx, side))
        def _():
            for d in range(nx):
                for x in x_edge(d, side):
                    x.wait() if d == 0 else x.wait_recv()

    def body_at(c):
        return pl.ds(pl.multiple_of(8 * c, 8), 8), pl.ds(8 * c - 2, 8)

    first_at = (pl.ds(2, 6), pl.ds(0, 6))

    acc[...] = jnp.zeros_like(acc)
    for side, at in ((0, slice(6, 8)), (1, slice(8 + rows, 10 + rows))):

        @pl.when(jnp.logical_not(has_edge(gx, side)))
        def _():
            E[1:5, :, at, :] = jnp.zeros_like(E[1:5, :, at, :])
            F[3, 1:5, :, at, :] = jnp.zeros_like(E[1:5, :, at, :])

    pl.semaphore_wait(bar, nx + 1)
    start_edges(0)
    start_tile(0)
    start_edges(1)
    for c in range(1, AHEAD):
        start_tile(c)
    wait_edges(0)

    def greet(r):
        for n in (2**r, ring - 2**r):
            to = lax.rem(m + n, ring)
            pl.semaphore_signal(
                tok.at[r], inc=1, device_id={"gy": lax.rem(to, ny), "gz": to // ny},
                device_id_type=MESH,
            )

    def start_z(at, c):
        for way in (0, 1):
            for x in z_window(way, at, c):
                x.start()

    def wait_z(at, c):
        for way in (0, 1):
            for x in z_window(way, at, c):
                x.wait_recv()

    def start_h(at, c):
        for way in (0, 1):
            h_window(way, at, c).start()

    def wait_h(at, c):
        for way in (0, 1):
            h_window(way, at, c).wait_recv()

    def z_at(c):
        return pl.ds(8 * c + 7, 8)

    def h_at(c):
        return pl.ds(pl.multiple_of(8 * c + 8, 8), 8)

    z_end, h_end = pl.ds(8 * tiles + 7, 2), pl.ds(8 * tiles + 8, 1)
    last = tiles - 1

    def step(c, _):
        @pl.when(c + AHEAD < tiles)
        def _():
            start_tile(c + AHEAD)

        for r in range(rounds):

            @pl.when(c == r)
            def _():
                if r > 0:
                    pl.semaphore_wait(tok.at[r - 1], 2)
                greet(r)

        @pl.when(c == rounds)
        def _():
            pl.semaphore_wait(tok.at[rounds - 1], 2)

        @pl.when(c == last)
        def _():
            wait_edges(1)

        wait_tile(c)
        start_z(z_at(c), c)

        @pl.when(c == last)
        def _():
            start_z(z_end, tiles)

        @pl.when(c >= 1)
        def _():
            wait_z(z_at(c - 1), c - 1)
            half(c - 1)
            start_h(h_at(c - 1), c - 1)

        @pl.when(c >= 2)
        def _():
            wait_h(h_at(c - 2), c - 2)
            full(c - 2)

        @pl.when(c == 4)
        def _():
            send_out(*first_at)
            send_out(*body_at(1))

        @pl.when(c >= 4)
        def _():
            send_out(*body_at(c - 2))

        return 0

    lax.fori_loop(0, tiles, step, 0)
    wait_z(z_at(last), last)
    wait_z(z_end, tiles)
    half(last)
    half(tiles)
    start_h(h_at(last), last)
    start_h(h_end, tiles)
    wait_h(h_at(last - 1), last - 1)
    full(last - 1)
    send_out(*body_at(last - 1))
    wait_h(h_at(last), last)
    wait_h(h_end, tiles)
    full(last)
    full(tiles)
    send_out(*body_at(last))
    send_out(pl.ds(8 * tiles, 2), pl.ds(rows - 2, 2))

    def meet(own, box, axis, size, me, send, recv):
        for d in range(1, size):
            copy(own, box.at[me], send.at[d], recv.at[d], {axis: lax.rem(me + d, size)}).start()
        for d in range(1, size):
            copy(own, box.at[me], send.at[d], recv.at[d], {axis: lax.rem(me + d, size)}).wait()

    part = jnp.sum(acc[...], axis=1)
    part = jnp.concatenate([part, jnp.zeros_like(part)], 0)
    SM[0] = part
    SA[gx] = part
    meet(SM.at[0], SA, "gx", nx, gx, sa_s, sa_r)
    part = SA[0]
    for i in range(1, nx):
        part = part + SA[i]
    SM[1] = part
    SB[gy] = part
    meet(SM.at[1], SB, "gy", ny, gy, sb_s, sb_r)
    planes = SB[...]
    total = jnp.sum(planes, axis=0)
    SM[2] = total
    SC[gz] = total
    meet(SM.at[2], SC, "gz", nz, gz, sc_s, sc_r)
    offset = jnp.zeros_like(total)
    for i in range(nz):
        offset = offset + jnp.where(i < gz, SC[i], 0.0)
    cells = 1.0 / (rows * nx * 128 * ny)
    run = jnp.sum(offset, axis=(0, 1), keepdims=True) * cells
    row = lax.broadcasted_iota(jnp.int32, (8, 128), 0)
    for g in range(ny):
        mean = jnp.broadcast_to(jnp.sum(planes[g], axis=1, keepdims=True) * cells, (8, 128))
        pm_ref[g] = mean
        upto = mean + jnp.where(row >= 1, pltpu.roll(mean, 1, 0), 0.0)
        upto = upto + jnp.where(row >= 2, pltpu.roll(upto, 2, 0), 0.0)
        rank = (row + (gz * 4 * ny + 4 * g + 1)).astype(jnp.float32)
        rm_ref[g] = (run + upto) / rank
        run = run + upto[3:4, 0:1]

    for d in range(ny):
        whole = o_ref.at[pl.ds(0, 4)]
        if d == 0:
            pltpu.make_async_copy(N.at[:, 0, pl.ds(0, rows), :], whole, orem.at[0]).wait()
        else:
            end = copy(
                N.at[:, 0, pl.ds(0, rows), :], whole, osem.at[d], orem.at[d],
                {"gy": lax.rem(gy + d, ny)},
            )
            end.wait()
    for d in range(1, nx):
        to = {"gx": lax.rem(gx + d, nx)}
        at = pl.ds(8, rows)
        copy(E.at[1, :, at, :], E.at[1, :, at, :], xsE.at[d], xrE.at[d, 0], to).wait_send()
        copy(F.at[:, 1, :, at, :], F.at[:, 1, :, at, :], xsF.at[d], xrF.at[d, 0], to).wait_send()
        for side in (0, 1):

            @pl.when(has_edge(lax.rem(gx + d, nx), side))
            def _():
                for x in x_edge(d, side):
                    x.wait_send()
    for way in (0, 1):
        for x in z_window(way, pl.ds(7, rows + 2), 0):
            x.wait_send()
        h_window(way, pl.ds(8, rows + 1), 0).wait_send()


def per_device(energy, flow):
    nx, ny, nz = (lax.axis_size(a) for a in ("gx", "gy", "gz"))
    e = energy.reshape(32, 8, 8, 128).transpose(0, 2, 1, 3)
    f = flow.reshape(4, 32, 8, 8, 128).transpose(0, 1, 3, 2, 4)
    vmem = pl.BlockSpec(memory_space=pltpu.VMEM)
    hbm = pl.BlockSpec(memory_space=pl.ANY)
    f32 = jnp.float32
    dma = pltpu.SemaphoreType.DMA
    result, mean, running = pl.pallas_call(
        functools.partial(kernel, nx, ny, nz),
        out_shape=(
            jax.ShapeDtypeStruct((32, 64, 128), f32),
            jax.ShapeDtypeStruct((8, 8, 128), f32),
            jax.ShapeDtypeStruct((8, 8, 128), f32),
        ),
        in_specs=[hbm, hbm],
        out_specs=(hbm, vmem, vmem),
        scratch_shapes=[
            pltpu.VMEM((6, 8, 88, 128), f32),
            pltpu.VMEM((4, 6, 8, 88, 128), f32),
            pltpu.VMEM((6, 8, 88, 128), f32),
            pltpu.VMEM((4, 8, 72, 128), f32),
            pltpu.VMEM((4, 8, 128), f32),
            pltpu.VMEM((4, 8, 128), f32),
            pltpu.VMEM((8, 8, 128), f32),
            pltpu.VMEM((8, 8, 128), f32),
            pltpu.VMEM((3, 8, 128), f32),
            dma((4,)), dma((4,)), dma((4, 8)), dma((4, 8)),
            dma((4, 2)), dma((4, 2)), dma((4, 2)), dma((4, 2)), dma((4, 2)), dma((4, 2)),
            dma((2,)), dma((2,)), dma((2,)), dma((2, 9)), dma((2, 9)), dma((2, 9)),
            dma((8,)), dma((8,)),
            dma((4,)), dma((4,)), dma((8,)), dma((8,)), dma((8,)), dma((8,)),
            pltpu.SemaphoreType.REGULAR((8,)),
        ],
        compiler_params=pltpu.CompilerParams(collective_id=0, has_side_effects=True),
        name="two_steps",
    )(e, f)
    return result, mean[:, :4, 0].reshape(-1), running[:, :4, 0].reshape(-1)


def solution(mesh):
    placed = (P(("gz", "gy", "gx"), None, None), P(None, ("gz", "gy", "gx"), None, None))
    return jax.shard_map(
        per_device,
        mesh=mesh,
        in_specs=placed,
        out_specs=(P("gz", "gx", "gy"), P("gz"), P("gz")),
        check_vma=False,
    )
```

```python
import functools

import jax
import jax.numpy as jnp
from jax import lax
from jax.experimental import pallas as pl
from jax.experimental.pallas import tpu as pltpu
from jax.sharding import PartitionSpec as P

MESH = pl.DeviceIdType.MESH
AHEAD = 3


def change_of(X, p, xi, F, fi):
    here = X[p, :, pl.ds(xi, 8), :]
    kappa = F[3, p, :, pl.ds(fi, 8), :]
    lane = lax.broadcasted_iota(jnp.int32, here.shape, 2)
    none = jnp.zeros_like(here[:1])

    def right(v):
        r = pltpu.roll(v, 127, 2)
        return jnp.where(lane == 127, jnp.concatenate([r[1:], none], 0), r)

    def left(v):
        r = pltpu.roll(v, 1, 2)
        return jnp.where(lane == 0, jnp.concatenate([none, r[:-1]], 0), r)

    sides = (
        (
            0,
            X[p + 1, :, pl.ds(xi, 8), :],
            F[3, p + 1, :, pl.ds(fi, 8), :],
            X[p - 1, :, pl.ds(xi, 8), :],
            F[3, p - 1, :, pl.ds(fi, 8), :],
        ),
        (
            1,
            X[p, :, pl.ds(xi + 1, 8), :],
            F[3, p, :, pl.ds(fi + 1, 8), :],
            X[p, :, pl.ds(xi - 1, 8), :],
            F[3, p, :, pl.ds(fi - 1, 8), :],
        ),
        (2, right(here), right(kappa), left(here), left(kappa)),
    )
    change = jnp.zeros_like(here)
    for axis, upper, kappa_upper, lower, kappa_lower in sides:
        speed = F[axis, p, :, pl.ds(fi, 8), :]
        change = (
            change
            + (0.5 * (kappa + kappa_upper) - jnp.minimum(speed, 0.0)) * (upper - here)
            - (0.5 * (kappa + kappa_lower) + jnp.maximum(speed, 0.0)) * (here - lower)
        )
    return here + change


def kernel(
    nx, ny, nz, e_ref, f_ref, o_ref, pm_ref, rm_ref, E, F, H, N, acc, SA, SC, SM,
    xsE, xsF, xrE, xrF, gsE, gsK, gsU, grE, grK, grU, zsE, zsK, zsH, zrE, zrK, zrH,
    osem, orem, sa_s, sa_r, sc_s, sc_r, tok,
):
    gx, gy, gz = (lax.axis_index(a) for a in ("gx", "gy", "gz"))
    ring = ny * nz
    m = gz * ny + gy
    up, down = lax.rem(m + 1, ring), lax.rem(m + ring - 1, ring)
    chain = tuple({"gy": lax.rem(n, ny), "gz": n // ny} for n in (up, down))
    rounds = (ring - 1).bit_length() - 1
    rows = 64
    tiles = rows // 8

    bar = pltpu.get_barrier_semaphore()
    for d in range(1, nx):
        pl.semaphore_signal(
            bar, inc=1, device_id={"gx": lax.rem(gx + d, nx)}, device_id_type=MESH
        )
    for to in chain:
        pl.semaphore_signal(bar, inc=1, device_id=to, device_id_type=MESH)

    def copy(src, dst, send, recv, to):
        return pltpu.make_async_remote_copy(
            src_ref=src, dst_ref=dst, send_sem=send, recv_sem=recv, device_id=to,
            device_id_type=MESH,
        )

    def x_tile(d, c):
        t = lax.rem(gx + d, nx)
        src = (e_ref.at[t * tiles + c], f_ref.at[:, t * tiles + c])
        at = pl.ds(pl.multiple_of(8 + 8 * c, 8), 8)
        dst = (E.at[1 + gx, :, at, :], F.at[:, 1 + gx, :, at, :])
        if d == 0:
            return (
                pltpu.make_async_copy(src[0], dst[0], xrE.at[0, c]),
                pltpu.make_async_copy(src[1], dst[1], xrF.at[0, c]),
            )
        return (
            copy(src[0], dst[0], xsE.at[d], xrE.at[d, c], {"gx": t}),
            copy(src[1], dst[1], xsF.at[d], xrF.at[d, c], {"gx": t}),
        )

    def x_edge(d, side):
        t = lax.rem(gx + d, nx)
        if side == 0:
            tile = lax.max(t * tiles - 1, 0)
            wide, narrow, wide_at, narrow_at = pl.ds(6, 2), pl.ds(7, 1), pl.ds(6, 2), pl.ds(7, 1)
        else:
            tile = lax.min((t + 1) * tiles, nx * tiles - 1)
            wide, narrow = pl.ds(0, 2), pl.ds(0, 1)
            wide_at, narrow_at = pl.ds(8 + rows, 2), pl.ds(8 + rows, 1)
        parts = (
            (e_ref.at[tile, :, wide, :], E.at[1 + gx, :, wide_at, :], gsE, grE),
            (f_ref.at[3, tile, :, wide, :], F.at[3, 1 + gx, :, wide_at, :], gsK, grK),
            (
                f_ref.at[pl.ds(0, 3), tile, :, narrow, :],
                F.at[pl.ds(0, 3), 1 + gx, :, narrow_at, :],
                gsU,
                grU,
            ),
        )
        if d == 0:
            return [pltpu.make_async_copy(a, b, r.at[0, side]) for a, b, s, r in parts]
        return [copy(a, b, s.at[d, side], r.at[d, side], {"gx": t}) for a, b, s, r in parts]

    def has_edge(g, side):
        return g > 0 if side == 0 else g < nx - 1

    def start_tile(c):
        for d in (0, *range(1, nx)):
            for x in x_tile(d, c):
                x.start()

    def start_edges(side):
        for d in range(nx):

            @pl.when(has_edge(lax.rem(gx + d, nx), side))
            def _():
                for x in x_edge(d, side):
                    x.start()

    def z_window(way, at, c):
        src, dst = ((4, 0), (1, 5))[way]
        return (
            copy(E.at[src, :, at, :], E.at[dst, :, at, :], zsE.at[way], zrE.at[way, c], chain[way]),
            copy(
                F.at[3, src, :, at, :], F.at[3, dst, :, at, :], zsK.at[way], zrK.at[way, c],
                chain[way],
            ),
        )

    def h_window(way, at, c):
        src, dst = ((4, 0), (1, 5))[way]
        return copy(
            H.at[src, :, at, :], H.at[dst, :, at, :], zsH.at[way], zrH.at[way, c], chain[way]
        )

    def out_window(d, src_at, dst_at):
        t = lax.rem(gy + d, ny)
        return copy(
            N.at[:, t, src_at, :], o_ref.at[pl.ds(4 * gy, 4), dst_at, :], osem.at[d], orem.at[d],
            {"gy": t},
        )

    def send_out(src_at, dst_at):
        def one(d, _):
            out_window(d, src_at, dst_at).start()
            return 0

        lax.fori_loop(1, ny, one, 0)
        pltpu.make_async_copy(
            N.at[:, gy, src_at, :], o_ref.at[pl.ds(4 * gy, 4), dst_at, :], orem.at[0]
        ).start()

    def half(c):
        def plane(p, _):
            v = change_of(E, p, 8 * c + 7, F, 8 * c + 7)
            r = lax.broadcasted_iota(jnp.int32, v.shape, 1) + (8 * c - 1 + rows * gx)
            H[p, :, pl.ds(pl.multiple_of(8 * c + 8, 8), 8), :] = jnp.where(
                (r >= 0) & (r < rows * nx), v, 0.0
            )
            return 0

        lax.fori_loop(1, 5, plane, 0)

    def full(c):
        def plane(p, _):
            v = change_of(H, p, 8 * c + 7, F, 8 * c + 6)
            N[p - 1, :, pl.ds(pl.multiple_of(8 * c, 8), 8), :] = v
            r = lax.broadcasted_iota(jnp.int32, v.shape, 1) + (8 * c - 2)
            acc[p - 1] += jnp.sum(jnp.where((r >= 0) & (r < rows), v, 0.0), axis=0)
            return 0

        lax.fori_loop(1, 5, plane, 0)

    def wait_tile(c):
        for d in range(nx):
            for x in x_tile(d, c):
                x.wait() if d == 0 else x.wait_recv()

    def wait_edges(side):
        @pl.when(has_edge(gx, side))
        def _():
            for d in range(nx):
                for x in x_edge(d, side):
                    x.wait() if d == 0 else x.wait_recv()

    def body_at(c):
        return pl.ds(pl.multiple_of(8 * c, 8), 8), pl.ds(8 * c - 2, 8)

    first_at = (pl.ds(2, 6), pl.ds(0, 6))

    acc[...] = jnp.zeros_like(acc)
    for side, at in ((0, slice(6, 8)), (1, slice(8 + rows, 10 + rows))):

        @pl.when(jnp.logical_not(has_edge(gx, side)))
        def _():
            E[1:5, :, at, :] = jnp.zeros_like(E[1:5, :, at, :])
            F[3, 1:5, :, at, :] = jnp.zeros_like(E[1:5, :, at, :])

    pl.semaphore_wait(bar, nx + 1)
    start_edges(0)
    start_tile(0)
    start_edges(1)
    for c in range(1, AHEAD):
        start_tile(c)
    wait_edges(0)

    def greet(r):
        for n in (2**r, ring - 2**r):
            to = lax.rem(m + n, ring)
            pl.semaphore_signal(
                tok.at[r], inc=1, device_id={"gy": lax.rem(to, ny), "gz": to // ny},
                device_id_type=MESH,
            )

    def start_z(at, c):
        for way in (0, 1):
            for x in z_window(way, at, c):
                x.start()

    def wait_z(at, c):
        for way in (0, 1):
            for x in z_window(way, at, c):
                x.wait_recv()

    def start_h(at, c):
        for way in (0, 1):
            h_window(way, at, c).start()

    def wait_h(at, c):
        for way in (0, 1):
            h_window(way, at, c).wait_recv()

    def z_at(c):
        return pl.ds(8 * c + 7, 8)

    def h_at(c):
        return pl.ds(pl.multiple_of(8 * c + 8, 8), 8)

    z_end, h_end = pl.ds(8 * tiles + 7, 2), pl.ds(8 * tiles + 8, 1)
    last = tiles - 1

    def step(c, _):
        @pl.when(c + AHEAD < tiles)
        def _():
            start_tile(c + AHEAD)

        for r in range(rounds):

            @pl.when(c == r)
            def _():
                if r > 0:
                    pl.semaphore_wait(tok.at[r - 1], 2)
                greet(r)

        @pl.when(c == rounds)
        def _():
            pl.semaphore_wait(tok.at[rounds - 1], 2)

        @pl.when(c == last)
        def _():
            wait_edges(1)

        wait_tile(c)
        start_z(z_at(c), c)

        @pl.when(c == last)
        def _():
            start_z(z_end, tiles)

        @pl.when(c >= 1)
        def _():
            wait_z(z_at(c - 1), c - 1)
            half(c - 1)
            start_h(h_at(c - 1), c - 1)

        @pl.when(c >= 2)
        def _():
            wait_h(h_at(c - 2), c - 2)
            full(c - 2)

        @pl.when(c == 4)
        def _():
            send_out(*first_at)
            send_out(*body_at(1))

        @pl.when(c >= 4)
        def _():
            send_out(*body_at(c - 2))

        return 0

    lax.fori_loop(0, tiles, step, 0)
    wait_z(z_at(last), last)
    wait_z(z_end, tiles)
    half(last)
    half(tiles)
    start_h(h_at(last), last)
    start_h(h_end, tiles)
    wait_h(h_at(last - 1), last - 1)
    full(last - 1)
    send_out(*body_at(last - 1))
    wait_h(h_at(last), last)
    wait_h(h_end, tiles)
    full(last)
    full(tiles)

    lane = lax.broadcasted_iota(jnp.int32, (1, 128), 1)
    part = jnp.zeros((1, 128), jnp.float32)
    for p in range(4):
        part = part + jnp.where(
            lane == 4 * gy + p, jnp.sum(acc[p], axis=(0, 1), keepdims=True), 0.0
        )
    SM[0] = part
    SA[gx * ny + gy] = part

    def group_row(n):
        to = lax.rem(gx * ny + gy + n, nx * ny)
        return copy(
            SM.at[0], SA.at[gx * ny + gy], sa_s.at[n], sa_r.at[n],
            {"gx": to // ny, "gy": lax.rem(to, ny)},
        )

    def start_row(n, _):
        group_row(n).start()
        return 0

    def wait_row(n, _):
        group_row(n).wait()
        return 0

    lax.fori_loop(1, nx * ny, start_row, 0)
    send_out(*body_at(last))
    send_out(pl.ds(8 * tiles, 2), pl.ds(rows - 2, 2))
    lax.fori_loop(1, nx * ny, wait_row, 0)
    planes = jnp.sum(SA[...], axis=0)
    SM[1] = planes

    def lift(d):
        return copy(SM.at[1], SC.at[gz], sc_s.at[d], sc_r.at[d], {"gz": lax.rem(gz + d, nz)})

    for d in range(1, nz):

        @pl.when(gz + d < nz)
        def _():
            lift(d).start()

    for d in range(1, nz):

        @pl.when(gz >= d)
        def _():
            lift(d).wait_recv()

    below = jnp.zeros_like(planes)
    for n in range(nz - 1):
        below = below + jnp.where(n < gz, SC[n], 0.0)
    cells = 1.0 / (rows * nx * 128 * ny)
    mean = jnp.broadcast_to(planes * cells, (8, 128))
    lane = lax.broadcasted_iota(jnp.int32, (8, 128), 1)
    upto = mean
    for n in (1, 2, 4, 8, 16):
        upto = upto + jnp.where(lane >= n, pltpu.roll(upto, n, 1), 0.0)
    rank = (lane + (gz * 4 * ny + 1)).astype(jnp.float32)
    pm_ref[...] = mean
    rm_ref[...] = (upto + jnp.sum(below, axis=(0, 1), keepdims=True) * cells) / rank
    for d in range(1, nz):

        @pl.when(gz + d < nz)
        def _():
            lift(d).wait_send()

    for d in range(ny):
        whole = o_ref.at[pl.ds(0, 4)]
        if d == 0:
            pltpu.make_async_copy(N.at[:, 0, pl.ds(0, rows), :], whole, orem.at[0]).wait()
        else:
            end = copy(
                N.at[:, 0, pl.ds(0, rows), :], whole, osem.at[d], orem.at[d],
                {"gy": lax.rem(gy + d, ny)},
            )
            end.wait()
    for d in range(1, nx):
        to = {"gx": lax.rem(gx + d, nx)}
        at = pl.ds(8, rows)
        copy(E.at[1, :, at, :], E.at[1, :, at, :], xsE.at[d], xrE.at[d, 0], to).wait_send()
        copy(F.at[:, 1, :, at, :], F.at[:, 1, :, at, :], xsF.at[d], xrF.at[d, 0], to).wait_send()
        for side in (0, 1):

            @pl.when(has_edge(lax.rem(gx + d, nx), side))
            def _():
                for x in x_edge(d, side):
                    x.wait_send()
    for way in (0, 1):
        for x in z_window(way, pl.ds(7, rows + 2), 0):
            x.wait_send()
        h_window(way, pl.ds(8, rows + 1), 0).wait_send()


def per_device(energy, flow):
    nx, ny, nz = (lax.axis_size(a) for a in ("gx", "gy", "gz"))
    e = energy.reshape(32, 8, 8, 128).transpose(0, 2, 1, 3)
    f = flow.reshape(4, 32, 8, 8, 128).transpose(0, 1, 3, 2, 4)
    vmem = pl.BlockSpec(memory_space=pltpu.VMEM)
    hbm = pl.BlockSpec(memory_space=pl.ANY)
    f32 = jnp.float32
    dma = pltpu.SemaphoreType.DMA
    result, mean, running = pl.pallas_call(
        functools.partial(kernel, nx, ny, nz),
        out_shape=(
            jax.ShapeDtypeStruct((32, 64, 128), f32),
            jax.ShapeDtypeStruct((8, 128), f32),
            jax.ShapeDtypeStruct((8, 128), f32),
        ),
        in_specs=[hbm, hbm],
        out_specs=(hbm, vmem, vmem),
        scratch_shapes=[
            pltpu.VMEM((6, 8, 88, 128), f32),
            pltpu.VMEM((4, 6, 8, 88, 128), f32),
            pltpu.VMEM((6, 8, 88, 128), f32),
            pltpu.VMEM((4, 8, 72, 128), f32),
            pltpu.VMEM((4, 8, 128), f32),
            pltpu.VMEM((32, 1, 128), f32),
            pltpu.VMEM((8, 1, 128), f32),
            pltpu.VMEM((2, 1, 128), f32),
            dma((4,)), dma((4,)), dma((4, 8)), dma((4, 8)),
            dma((4, 2)), dma((4, 2)), dma((4, 2)), dma((4, 2)), dma((4, 2)), dma((4, 2)),
            dma((2,)), dma((2,)), dma((2,)), dma((2, 9)), dma((2, 9)), dma((2, 9)),
            dma((8,)), dma((8,)),
            dma((32,)), dma((32,)), dma((8,)), dma((8,)),
            pltpu.SemaphoreType.REGULAR((8,)),
        ],
        compiler_params=pltpu.CompilerParams(collective_id=0, has_side_effects=True),
        name="two_steps",
    )(e, f)
    return result, mean[0, :32], running[0, :32]


def solution(mesh):
    placed = (P(("gz", "gy", "gx"), None, None), P(None, ("gz", "gy", "gx"), None, None))
    return jax.shard_map(
        per_device,
        mesh=mesh,
        in_specs=placed,
        out_specs=(P("gz", "gx", "gy"), P("gz"), P("gz")),
        check_vma=False,
    )
```

```python
import functools

import jax
import jax.numpy as jnp
from jax import lax
from jax.experimental import pallas as pl
from jax.experimental.pallas import tpu as pltpu
from jax.sharding import PartitionSpec as P

MESH = pl.DeviceIdType.MESH
AHEAD = 3


def change_of(X, p, xi, F, fi):
    here = X[p, :, pl.ds(xi, 8), :]
    kappa = F[3, p, :, pl.ds(fi, 8), :]
    lane = lax.broadcasted_iota(jnp.int32, here.shape, 2)
    none = jnp.zeros_like(here[:1])

    def right(v):
        r = pltpu.roll(v, 127, 2)
        return jnp.where(lane == 127, jnp.concatenate([r[1:], none], 0), r)

    def left(v):
        r = pltpu.roll(v, 1, 2)
        return jnp.where(lane == 0, jnp.concatenate([none, r[:-1]], 0), r)

    sides = (
        (
            0,
            X[p + 1, :, pl.ds(xi, 8), :],
            F[3, p + 1, :, pl.ds(fi, 8), :],
            X[p - 1, :, pl.ds(xi, 8), :],
            F[3, p - 1, :, pl.ds(fi, 8), :],
        ),
        (
            1,
            X[p, :, pl.ds(xi + 1, 8), :],
            F[3, p, :, pl.ds(fi + 1, 8), :],
            X[p, :, pl.ds(xi - 1, 8), :],
            F[3, p, :, pl.ds(fi - 1, 8), :],
        ),
        (2, right(here), right(kappa), left(here), left(kappa)),
    )
    change = jnp.zeros_like(here)
    for axis, upper, kappa_upper, lower, kappa_lower in sides:
        speed = F[axis, p, :, pl.ds(fi, 8), :]
        change = (
            change
            + (0.5 * (kappa + kappa_upper) - jnp.minimum(speed, 0.0)) * (upper - here)
            - (0.5 * (kappa + kappa_lower) + jnp.maximum(speed, 0.0)) * (here - lower)
        )
    return here + change


def kernel(
    nx, ny, nz, e_ref, f_ref, o_ref, pm_ref, rm_ref, E, F, H, N, acc, SA, SC, SM,
    xsE, xsF, xrE, xrF, gsE, gsK, gsU, grE, grK, grU, zsE, zsK, zsH, zrE, zrK, zrH,
    osem, orem, sa_s, sa_r, sc_s, sc_r, tok,
):
    gx, gy, gz = (lax.axis_index(a) for a in ("gx", "gy", "gz"))
    ring = ny * nz
    m = gz * ny + gy
    up, down = lax.rem(m + 1, ring), lax.rem(m + ring - 1, ring)
    chain = tuple({"gy": lax.rem(n, ny), "gz": n // ny} for n in (up, down))
    rounds = (ring - 1).bit_length() - 1
    rows = 64
    tiles = rows // 8

    bar = pltpu.get_barrier_semaphore()
    for d in range(1, nx):
        pl.semaphore_signal(
            bar, inc=1, device_id={"gx": lax.rem(gx + d, nx)}, device_id_type=MESH
        )
    for to in chain:
        pl.semaphore_signal(bar, inc=1, device_id=to, device_id_type=MESH)

    def copy(src, dst, send, recv, to):
        return pltpu.make_async_remote_copy(
            src_ref=src, dst_ref=dst, send_sem=send, recv_sem=recv, device_id=to,
            device_id_type=MESH,
        )

    def x_rows(d, part, c):
        t = lax.rem(gx + d, nx)
        inside = (pl.ds(0, 2), pl.ds(2, 6))[part]
        at = pl.ds(8 + 8 * c + 2 * part, (2, 6)[part])
        parts = (
            (e_ref.at[t * tiles + c, :, inside, :], E.at[1 + gx, :, at, :], xsE, xrE),
            (f_ref.at[:, t * tiles + c, :, inside, :], F.at[:, 1 + gx, :, at, :], xsF, xrF),
        )
        if d == 0:
            return [pltpu.make_async_copy(a, b, r.at[part, 0, c]) for a, b, s, r in parts]
        return [copy(a, b, s.at[d], r.at[part, d, c], {"gx": t}) for a, b, s, r in parts]

    def x_edge(d, side):
        t = lax.rem(gx + d, nx)
        if side == 0:
            tile = lax.max(t * tiles - 1, 0)
            wide, narrow, wide_at, narrow_at = pl.ds(6, 2), pl.ds(7, 1), pl.ds(6, 2), pl.ds(7, 1)
        else:
            tile = lax.min((t + 1) * tiles, nx * tiles - 1)
            wide, narrow = pl.ds(0, 2), pl.ds(0, 1)
            wide_at, narrow_at = pl.ds(8 + rows, 2), pl.ds(8 + rows, 1)
        parts = (
            (e_ref.at[tile, :, wide, :], E.at[1 + gx, :, wide_at, :], gsE, grE),
            (f_ref.at[3, tile, :, wide, :], F.at[3, 1 + gx, :, wide_at, :], gsK, grK),
            (
                f_ref.at[pl.ds(0, 3), tile, :, narrow, :],
                F.at[pl.ds(0, 3), 1 + gx, :, narrow_at, :],
                gsU,
                grU,
            ),
        )
        if d == 0:
            return [pltpu.make_async_copy(a, b, r.at[0, side]) for a, b, s, r in parts]
        return [copy(a, b, s.at[d, side], r.at[d, side], {"gx": t}) for a, b, s, r in parts]

    def has_edge(g, side):
        return g > 0 if side == 0 else g < nx - 1

    def start_rows(part, c):
        for d in range(nx):
            for x in x_rows(d, part, c):
                x.start()

    def start_tile(c):
        start_rows(1, c)

        @pl.when(c < tiles - 1)
        def _():
            start_rows(0, lax.min(c + 1, tiles - 1))

    def start_edges(side):
        for d in range(nx):

            @pl.when(has_edge(lax.rem(gx + d, nx), side))
            def _():
                for x in x_edge(d, side):
                    x.start()

    def z_window(way, at, c):
        src, dst = ((4, 0), (1, 5))[way]
        return (
            copy(E.at[src, :, at, :], E.at[dst, :, at, :], zsE.at[way], zrE.at[way, c], chain[way]),
            copy(
                F.at[3, src, :, at, :], F.at[3, dst, :, at, :], zsK.at[way], zrK.at[way, c],
                chain[way],
            ),
        )

    def h_window(way, at, c):
        src, dst = ((4, 0), (1, 5))[way]
        return copy(
            H.at[src, :, at, :], H.at[dst, :, at, :], zsH.at[way], zrH.at[way, c], chain[way]
        )

    def out_window(d, at):
        t = lax.rem(gy + d, ny)
        return copy(
            N.at[:, t, at, :], o_ref.at[pl.ds(4 * gy, 4), at, :], osem.at[d], orem.at[d],
            {"gy": t},
        )

    def send_out(at):
        def one(d, _):
            out_window(d, at).start()
            return 0

        lax.fori_loop(1, ny, one, 0)
        pltpu.make_async_copy(
            N.at[:, gy, at, :], o_ref.at[pl.ds(4 * gy, 4), at, :], orem.at[0]
        ).start()

    def over(planes, work):
        def one(n, _):
            work(planes[0] + (planes[1] - planes[0]) * n)
            return 0

        lax.fori_loop(0, 2, one, 0)

    inner, outer = (2, 3), (1, 4)

    def half(c, planes):
        def plane(p):
            v = change_of(E, p, 8 * c + 9, F, 8 * c + 9)
            r = lax.broadcasted_iota(jnp.int32, v.shape, 1) + (8 * c + 1 + rows * gx)
            H[p, :, pl.ds(pl.multiple_of(8 * c + 8, 8), 8), :] = jnp.where(
                (r >= 0) & (r < rows * nx), v, 0.0
            )

        over(planes, plane)

    def full(c, planes):
        def plane(p):
            v = change_of(H, p, 8 * c + 7, F, pl.multiple_of(8 * c + 8, 8))
            N[p - 1, :, pl.ds(pl.multiple_of(8 * c, 8), 8), :] = v
            acc[p - 1] += jnp.sum(v, axis=0)

        over(planes, plane)

    def wait_rows(part, c):
        for d in range(nx):
            for x in x_rows(d, part, c):
                x.wait() if d == 0 else x.wait_recv()

    def wait_tile(c):
        wait_rows(1, c)

        @pl.when(c < tiles - 1)
        def _():
            wait_rows(0, lax.min(c + 1, tiles - 1))

    def wait_edges(side):
        @pl.when(has_edge(gx, side))
        def _():
            for d in range(nx):
                for x in x_edge(d, side):
                    x.wait() if d == 0 else x.wait_recv()

    def out_at(c):
        return pl.ds(pl.multiple_of(8 * c, 8), 8)

    acc[...] = jnp.zeros_like(acc)
    for side, at in ((0, slice(6, 8)), (1, slice(8 + rows, 10 + rows))):

        @pl.when(jnp.logical_not(has_edge(gx, side)))
        def _():
            E[1:5, :, at, :] = jnp.zeros_like(E[1:5, :, at, :])
            F[3, 1:5, :, at, :] = jnp.zeros_like(E[1:5, :, at, :])

    pl.semaphore_wait(bar, nx + 1)
    start_edges(0)
    start_rows(0, 0)
    start_tile(0)
    start_edges(1)
    for c in range(1, AHEAD):
        start_tile(c)
    wait_edges(0)
    wait_rows(0, 0)

    def greet(r):
        for n in (2**r, ring - 2**r):
            to = lax.rem(m + n, ring)
            pl.semaphore_signal(
                tok.at[r], inc=1, device_id={"gy": lax.rem(to, ny), "gz": to // ny},
                device_id_type=MESH,
            )

    def start_z(at, c):
        for way in (0, 1):
            for x in z_window(way, at, c):
                x.start()

    def wait_z(at, c):
        for way in (0, 1):
            for x in z_window(way, at, c):
                x.wait_recv()

    def start_h(at, c):
        for way in (0, 1):
            h_window(way, at, c).start()

    def wait_h(at, c):
        for way in (0, 1):
            h_window(way, at, c).wait_recv()

    def z_at(c):
        return pl.ds(8 * c + 9, 8)

    def h_at(c):
        return pl.ds(pl.multiple_of(8 * c + 8, 8), 8)

    z_first, h_first = pl.ds(7, 2), pl.ds(7, 1)
    last = tiles - 1
    start_z(z_first, tiles)

    def step(c, _):
        @pl.when(c + AHEAD < tiles)
        def _():
            start_tile(c + AHEAD)

        for r in range(rounds):

            @pl.when(c == r)
            def _():
                if r > 0:
                    pl.semaphore_wait(tok.at[r - 1], 2)
                greet(r)

        @pl.when(c == rounds)
        def _():
            pl.semaphore_wait(tok.at[rounds - 1], 2)

        @pl.when(c == last)
        def _():
            wait_edges(1)

        wait_tile(c)
        start_z(z_at(c), c)

        @pl.when(c == 1)
        def _():
            wait_z(z_first, tiles)
            half(-1, inner)
            half(-1, outer)
            start_h(h_first, tiles)

        @pl.when(c >= 1)
        def _():
            half(c - 1, inner)
            wait_z(z_at(c - 1), c - 1)
            half(c - 1, outer)
            start_h(h_at(c - 1), c - 1)

        @pl.when(c == 2)
        def _():
            wait_h(h_first, tiles)

        @pl.when(c >= 2)
        def _():
            full(c - 2, inner)
            wait_h(h_at(c - 2), c - 2)
            full(c - 2, outer)

        @pl.when(c == 4)
        def _():
            send_out(out_at(0))
            send_out(out_at(1))

        @pl.when(c >= 4)
        def _():
            send_out(out_at(c - 2))

        return 0

    lax.fori_loop(0, tiles, step, 0)
    half(last, inner)
    wait_z(z_at(last), last)
    half(last, outer)
    start_h(h_at(last), last)
    full(last - 1, inner)
    wait_h(h_at(last - 1), last - 1)
    full(last - 1, outer)
    send_out(out_at(last - 1))
    full(last, inner)
    wait_h(h_at(last), last)
    full(last, outer)

    lane = lax.broadcasted_iota(jnp.int32, (1, 128), 1)
    part = jnp.zeros((1, 128), jnp.float32)
    for p in range(4):
        part = part + jnp.where(
            lane == 4 * gy + p, jnp.sum(acc[p], axis=(0, 1), keepdims=True), 0.0
        )
    SM[0] = part
    SA[gx * ny + gy] = part

    def group_row(n):
        to = lax.rem(gx * ny + gy + n, nx * ny)
        return copy(
            SM.at[0], SA.at[gx * ny + gy], sa_s.at[n], sa_r.at[n],
            {"gx": to // ny, "gy": lax.rem(to, ny)},
        )

    def start_row(n, _):
        group_row(n).start()
        return 0

    def wait_row(n, _):
        group_row(n).wait()
        return 0

    lax.fori_loop(1, nx * ny, start_row, 0)
    send_out(out_at(last))
    lax.fori_loop(1, nx * ny, wait_row, 0)
    planes = jnp.sum(SA[...], axis=0)
    SM[1] = planes

    def lift(to_z, to_y, slot):
        return copy(
            SM.at[1], SC.at[gz], sc_s.at[to_z, slot], sc_r.at[gz], {"gy": to_y, "gz": to_z}
        )

    def lifts(act):
        for to in range(1, nz):
            alike = lax.rem(gz + to, 2) == 0

            @pl.when((gz < to) & alike)
            def _():
                act(lift(to, gy, 0))

            for end, first in ((ny - 1, 0), (1, ny // 2)):

                @pl.when((gz < to) & jnp.logical_not(alike) & (gy == end))
                def _():
                    for n in range(ny // 2):
                        act(lift(to, first + n, n))

    lifts(lambda x: x.start())
    for n in range(nz - 1):

        @pl.when(n < gz)
        def _():
            copy(SM.at[1], SC.at[n], sc_s.at[0, 0], sc_r.at[n], {"gz": gz}).wait_recv()

    below = jnp.zeros_like(planes)
    for n in range(nz - 1):
        below = below + jnp.where(n < gz, SC[n], 0.0)
    cells = 1.0 / (rows * nx * 128 * ny)
    mean = jnp.broadcast_to(planes * cells, (8, 128))
    lane = lax.broadcasted_iota(jnp.int32, (8, 128), 1)
    upto = mean
    for n in (1, 2, 4, 8, 16):
        upto = upto + jnp.where(lane >= n, pltpu.roll(upto, n, 1), 0.0)
    rank = (lane + (gz * 4 * ny + 1)).astype(jnp.float32)
    pm_ref[...] = mean
    rm_ref[...] = (upto + jnp.sum(below, axis=(0, 1), keepdims=True) * cells) / rank
    lifts(lambda x: x.wait_send())

    for d in range(ny):
        whole = o_ref.at[pl.ds(0, 4)]
        if d == 0:
            pltpu.make_async_copy(N.at[:, 0, pl.ds(0, rows), :], whole, orem.at[0]).wait()
        else:
            end = copy(
                N.at[:, 0, pl.ds(0, rows), :], whole, osem.at[d], orem.at[d],
                {"gy": lax.rem(gy + d, ny)},
            )
            end.wait()
    for d in range(1, nx):
        to = {"gx": lax.rem(gx + d, nx)}
        at = pl.ds(8, rows)
        copy(E.at[1, :, at, :], E.at[1, :, at, :], xsE.at[d], xrE.at[0, d, 0], to).wait_send()
        copy(F.at[:, 1, :, at, :], F.at[:, 1, :, at, :], xsF.at[d], xrF.at[0, d, 0], to).wait_send()
        for side in (0, 1):

            @pl.when(has_edge(lax.rem(gx + d, nx), side))
            def _():
                for x in x_edge(d, side):
                    x.wait_send()
    for way in (0, 1):
        for x in z_window(way, pl.ds(7, rows + 2), 0):
            x.wait_send()
        h_window(way, pl.ds(7, rows + 1), 0).wait_send()


def per_device(energy, flow):
    nx, ny, nz = (lax.axis_size(a) for a in ("gx", "gy", "gz"))
    e = energy.reshape(32, 8, 8, 128).transpose(0, 2, 1, 3)
    f = flow.reshape(4, 32, 8, 8, 128).transpose(0, 1, 3, 2, 4)
    vmem = pl.BlockSpec(memory_space=pltpu.VMEM)
    hbm = pl.BlockSpec(memory_space=pl.ANY)
    f32 = jnp.float32
    dma = pltpu.SemaphoreType.DMA
    result, mean, running = pl.pallas_call(
        functools.partial(kernel, nx, ny, nz),
        out_shape=(
            jax.ShapeDtypeStruct((32, 64, 128), f32),
            jax.ShapeDtypeStruct((8, 128), f32),
            jax.ShapeDtypeStruct((8, 128), f32),
        ),
        in_specs=[hbm, hbm],
        out_specs=(hbm, vmem, vmem),
        scratch_shapes=[
            pltpu.VMEM((6, 8, 80, 128), f32),
            pltpu.VMEM((4, 6, 8, 80, 128), f32),
            pltpu.VMEM((6, 8, 80, 128), f32),
            pltpu.VMEM((4, 8, 64, 128), f32),
            pltpu.VMEM((4, 8, 128), f32),
            pltpu.VMEM((32, 1, 128), f32),
            pltpu.VMEM((8, 1, 128), f32),
            pltpu.VMEM((2, 1, 128), f32),
            dma((4,)), dma((4,)), dma((2, 4, 8)), dma((2, 4, 8)),
            dma((4, 2)), dma((4, 2)), dma((4, 2)), dma((4, 2)), dma((4, 2)), dma((4, 2)),
            dma((2,)), dma((2,)), dma((2,)), dma((2, 9)), dma((2, 9)), dma((2, 9)),
            dma((8,)), dma((8,)),
            dma((32,)), dma((32,)), dma((8, 4)), dma((8,)),
            pltpu.SemaphoreType.REGULAR((8,)),
        ],
        compiler_params=pltpu.CompilerParams(
            collective_id=0, has_side_effects=True, vmem_limit_bytes=55_000_000
        ),
        name="two_steps",
    )(e, f)
    return result, mean[0, :32], running[0, :32]


def solution(mesh):
    placed = (P(("gz", "gy", "gx"), None, None), P(None, ("gz", "gy", "gx"), None, None))
    return jax.shard_map(
        per_device,
        mesh=mesh,
        in_specs=placed,
        out_specs=(P("gz", "gx", "gy"), P("gz"), P("gz")),
        check_vma=False,
    )
```

```python
import functools

import jax
import jax.numpy as jnp
from jax import lax
from jax.experimental import pallas as pl
from jax.experimental.pallas import tpu as pltpu
from jax.sharding import PartitionSpec as P

MESH = pl.DeviceIdType.MESH
AHEAD = 3


def change_of(X, p, xi, F, fi):
    here = X[p, :, pl.ds(xi, 8), :]
    kappa = F[3, p, :, pl.ds(fi, 8), :]
    lane = lax.broadcasted_iota(jnp.int32, here.shape, 2)
    none = jnp.zeros_like(here[:1])

    def right(v):
        r = pltpu.roll(v, 127, 2)
        return jnp.where(lane == 127, jnp.concatenate([r[1:], none], 0), r)

    def left(v):
        r = pltpu.roll(v, 1, 2)
        return jnp.where(lane == 0, jnp.concatenate([none, r[:-1]], 0), r)

    sides = (
        (
            0,
            X[p + 1, :, pl.ds(xi, 8), :],
            F[3, p + 1, :, pl.ds(fi, 8), :],
            X[p - 1, :, pl.ds(xi, 8), :],
            F[3, p - 1, :, pl.ds(fi, 8), :],
        ),
        (
            1,
            X[p, :, pl.ds(xi + 1, 8), :],
            F[3, p, :, pl.ds(fi + 1, 8), :],
            X[p, :, pl.ds(xi - 1, 8), :],
            F[3, p, :, pl.ds(fi - 1, 8), :],
        ),
        (2, right(here), right(kappa), left(here), left(kappa)),
    )
    change = jnp.zeros_like(here)
    for axis, upper, kappa_upper, lower, kappa_lower in sides:
        speed = F[axis, p, :, pl.ds(fi, 8), :]
        change = (
            change
            + (0.5 * (kappa + kappa_upper) - jnp.minimum(speed, 0.0)) * (upper - here)
            - (0.5 * (kappa + kappa_lower) + jnp.maximum(speed, 0.0)) * (here - lower)
        )
    return here + change


def kernel(
    nx, ny, nz, e_ref, f_ref, o_ref, pm_ref, rm_ref, E, F, H, N, acc, SA, SC, SM,
    xsE, xsF, xrE, xrF, gsE, gsK, grE, grK, xsH, xrH, zsE, zsK, zsH, zrE, zrK, zrH,
    osem, orem, sa_s, sa_r, sc_s, sc_r, tok,
):
    gx, gy, gz = (lax.axis_index(a) for a in ("gx", "gy", "gz"))
    ring = ny * nz
    m = gz * ny + gy
    up, down = lax.rem(m + 1, ring), lax.rem(m + ring - 1, ring)
    chain = tuple({"gy": lax.rem(n, ny), "gz": n // ny} for n in (up, down))
    rounds = (ring - 1).bit_length() - 1
    rows = 64
    tiles = rows // 8

    bar = pltpu.get_barrier_semaphore()
    for d in range(1, nx):
        pl.semaphore_signal(
            bar, inc=1, device_id={"gx": lax.rem(gx + d, nx)}, device_id_type=MESH
        )
    for to in chain:
        pl.semaphore_signal(bar, inc=1, device_id=to, device_id_type=MESH)

    def copy(src, dst, send, recv, to):
        return pltpu.make_async_remote_copy(
            src_ref=src, dst_ref=dst, send_sem=send, recv_sem=recv, device_id=to,
            device_id_type=MESH,
        )

    def x_rows(d, part, c):
        t = lax.rem(gx + d, nx)
        inside = (pl.ds(0, 2), pl.ds(2, 6))[part]
        at = pl.ds(8 + 8 * c + 2 * part, (2, 6)[part])
        parts = (
            (e_ref.at[t * tiles + c, :, inside, :], E.at[1 + gx, :, at, :], xsE, xrE),
            (f_ref.at[:, t * tiles + c, :, inside, :], F.at[:, 1 + gx, :, at, :], xsF, xrF),
        )
        if d == 0:
            return [pltpu.make_async_copy(a, b, r.at[part, 0, c]) for a, b, s, r in parts]
        return [copy(a, b, s.at[d], r.at[part, d, c], {"gx": t}) for a, b, s, r in parts]

    def x_edge(d, side):
        t = lax.rem(gx + d, nx)
        if side == 0:
            tile, row, at = lax.max(t * tiles - 1, 0), pl.ds(7, 1), pl.ds(7, 1)
        else:
            tile, row, at = lax.min((t + 1) * tiles, nx * tiles - 1), pl.ds(0, 1), pl.ds(8 + rows, 1)
        parts = (
            (e_ref.at[tile, :, row, :], E.at[1 + gx, :, at, :], gsE, grE),
            (f_ref.at[3, tile, :, row, :], F.at[3, 1 + gx, :, at, :], gsK, grK),
        )
        if d == 0:
            return [pltpu.make_async_copy(a, b, r.at[0, side]) for a, b, s, r in parts]
        return [copy(a, b, s.at[d, side], r.at[d, side], {"gx": t}) for a, b, s, r in parts]

    def x_half(side):
        src, dst = ((7, 71), (70, 6))[side]
        return copy(
            H.at[pl.ds(1, 4), :, pl.ds(src, 1), :], H.at[pl.ds(1, 4), :, pl.ds(dst, 1), :],
            xsH.at[side], xrH.at[side], {"gx": lax.rem(gx + (nx - 1, 1)[side], nx)},
        )

    def has_edge(g, side):
        return g > 0 if side == 0 else g < nx - 1

    def start_rows(part, c):
        for d in range(nx):
            for x in x_rows(d, part, c):
                x.start()

    def start_tile(c):
        start_rows(1, c)

        @pl.when(c < tiles - 1)
        def _():
            start_rows(0, lax.min(c + 1, tiles - 1))

    def start_edges(side):
        for d in range(nx):

            @pl.when(has_edge(lax.rem(gx + d, nx), side))
            def _():
                for x in x_edge(d, side):
                    x.start()

    def z_window(way, at, c):
        src, dst = ((4, 0), (1, 5))[way]
        return (
            copy(E.at[src, :, at, :], E.at[dst, :, at, :], zsE.at[way], zrE.at[way, c], chain[way]),
            copy(
                F.at[3, src, :, at, :], F.at[3, dst, :, at, :], zsK.at[way], zrK.at[way, c],
                chain[way],
            ),
        )

    def h_window(way, at, c):
        src, dst = ((4, 0), (1, 5))[way]
        return copy(
            H.at[src, :, at, :], H.at[dst, :, at, :], zsH.at[way], zrH.at[way, c], chain[way]
        )

    def out_window(d, at):
        t = lax.rem(gy + d, ny)
        return copy(
            N.at[:, t, at, :], o_ref.at[pl.ds(4 * gy, 4), at, :], osem.at[d], orem.at[d],
            {"gy": t},
        )

    def send_out(at):
        def one(d, _):
            out_window(d, at).start()
            return 0

        lax.fori_loop(1, ny, one, 0)
        pltpu.make_async_copy(
            N.at[:, gy, at, :], o_ref.at[pl.ds(4 * gy, 4), at, :], orem.at[0]
        ).start()

    def over(planes, work):
        def one(n, _):
            work(planes[0] + (planes[1] - planes[0]) * n)
            return 0

        lax.fori_loop(0, 2, one, 0)

    inner, outer = (2, 3), (1, 4)

    def half(c, planes, first=0, count=8):
        def plane(p):
            v = change_of(E, p, 8 * c + 9, F, 8 * c + 9)
            at = 8 * c + 8 + first if count < 8 else pl.multiple_of(8 * c + 8, 8)
            H[p, :, pl.ds(at, count), :] = v[:, first : first + count]

        over(planes, plane)

    def full(c, planes):
        def plane(p):
            v = change_of(H, p, 8 * c + 7, F, pl.multiple_of(8 * c + 8, 8))
            N[p - 1, :, pl.ds(pl.multiple_of(8 * c, 8), 8), :] = v
            acc[p - 1] += jnp.sum(v, axis=0)

        over(planes, plane)

    def wait_rows(part, c):
        for d in range(nx):
            for x in x_rows(d, part, c):
                x.wait() if d == 0 else x.wait_recv()

    def wait_tile(c):
        wait_rows(1, c)

        @pl.when(c < tiles - 1)
        def _():
            wait_rows(0, lax.min(c + 1, tiles - 1))

    def wait_edges(side):
        @pl.when(has_edge(gx, side))
        def _():
            for d in range(nx):
                for x in x_edge(d, side):
                    x.wait() if d == 0 else x.wait_recv()

    def out_at(c):
        return pl.ds(pl.multiple_of(8 * c, 8), 8)

    acc[...] = jnp.zeros_like(acc)
    for side, at, half_at in ((0, 7, 6), (1, 8 + rows, 7 + rows)):

        @pl.when(jnp.logical_not(has_edge(gx, side)))
        def _():
            none = jnp.zeros((4, ny, 1, 128), jnp.float32)
            E[1:5, :, at : at + 1, :] = none
            F[3, 1:5, :, at : at + 1, :] = none
            H[1:5, :, half_at : half_at + 1, :] = none

    pl.semaphore_wait(bar, nx + 1)
    start_edges(0)
    start_rows(0, 0)
    start_tile(0)
    start_edges(1)
    for c in range(1, AHEAD):
        start_tile(c)
    wait_edges(0)
    wait_rows(0, 0)

    def greet(r):
        for n in (2**r, ring - 2**r):
            to = lax.rem(m + n, ring)
            pl.semaphore_signal(
                tok.at[r], inc=1, device_id={"gy": lax.rem(to, ny), "gz": to // ny},
                device_id_type=MESH,
            )

    def start_z(at, c):
        for way in (0, 1):
            for x in z_window(way, at, c):
                x.start()

    def wait_z(at, c):
        for way in (0, 1):
            for x in z_window(way, at, c):
                x.wait_recv()

    def start_h(at, c):
        for way in (0, 1):
            h_window(way, at, c).start()

    def wait_h(at, c):
        for way in (0, 1):
            h_window(way, at, c).wait_recv()

    def z_at(c):
        return pl.ds(8 * c + 9, 8)

    def h_at(c):
        return pl.ds(pl.multiple_of(8 * c + 8, 8), 8)

    z_first, h_first = pl.ds(8, 1), pl.ds(7, 1)
    last = tiles - 1
    h_last = pl.ds(8 * last + 8, 7)
    start_z(z_first, tiles)

    def step(c, _):
        @pl.when(c + AHEAD < tiles)
        def _():
            start_tile(c + AHEAD)

        for r in range(rounds):

            @pl.when(c == r)
            def _():
                if r > 0:
                    pl.semaphore_wait(tok.at[r - 1], 2)
                greet(r)

        @pl.when(c == rounds)
        def _():
            pl.semaphore_wait(tok.at[rounds - 1], 2)

        @pl.when(c == last)
        def _():
            wait_edges(1)

        wait_tile(c)
        start_z(z_at(c), c)

        @pl.when(c == 1)
        def _():
            wait_z(z_first, tiles)
            half(-1, inner, 7, 1)
            half(-1, outer, 7, 1)
            start_h(h_first, tiles)

            @pl.when(has_edge(gx, 0))
            def _():
                x_half(0).start()

        @pl.when(c >= 1)
        def _():
            half(c - 1, inner)
            wait_z(z_at(c - 1), c - 1)
            half(c - 1, outer)
            start_h(h_at(c - 1), c - 1)

        @pl.when(c == 2)
        def _():
            wait_h(h_first, tiles)

        @pl.when(c == 2)
        def _():
            wait_h(h_at(0), 0)

        @pl.when(c >= 3)
        def _():
            full(c - 2, inner)
            wait_h(h_at(c - 2), c - 2)
            full(c - 2, outer)

        @pl.when(c == 4)
        def _():
            send_out(out_at(1))

        @pl.when(c >= 4)
        def _():
            send_out(out_at(c - 2))

        return 0

    lax.fori_loop(0, tiles, step, 0)
    half(last, inner, 0, 7)
    wait_z(z_at(last), last)
    half(last, outer, 0, 7)
    start_h(h_last, last)

    @pl.when(has_edge(gx, 1))
    def _():
        x_half(1).start()

    full(last - 1, inner)
    wait_h(h_at(last - 1), last - 1)
    full(last - 1, outer)
    send_out(out_at(last - 1))

    @pl.when(has_edge(gx, 1))
    def _():
        x_half(0).wait_recv()

    full(last, inner)
    wait_h(h_last, last)
    full(last, outer)

    @pl.when(has_edge(gx, 0))
    def _():
        x_half(1).wait_recv()

    full(0, inner)
    full(0, outer)

    lane = lax.broadcasted_iota(jnp.int32, (1, 128), 1)
    part = jnp.zeros((1, 128), jnp.float32)
    for p in range(4):
        part = part + jnp.where(
            lane == 4 * gy + p, jnp.sum(acc[p], axis=(0, 1), keepdims=True), 0.0
        )
    SM[0] = part
    SA[gx * ny + gy] = part

    def group_row(n):
        to = lax.rem(gx * ny + gy + n, nx * ny)
        return copy(
            SM.at[0], SA.at[gx * ny + gy], sa_s.at[n], sa_r.at[n],
            {"gx": to // ny, "gy": lax.rem(to, ny)},
        )

    def start_row(n, _):
        group_row(n).start()
        return 0

    def wait_row(n, _):
        group_row(n).wait()
        return 0

    lax.fori_loop(1, nx * ny, start_row, 0)
    send_out(out_at(last))
    send_out(out_at(0))
    lax.fori_loop(1, nx * ny, wait_row, 0)
    planes = jnp.sum(SA[...], axis=0)
    SM[1] = planes

    def lift(to_z, to_y, slot):
        return copy(
            SM.at[1], SC.at[gz], sc_s.at[to_z, slot], sc_r.at[gz], {"gy": to_y, "gz": to_z}
        )

    def lifts(act):
        for to in range(1, nz):
            alike = lax.rem(gz + to, 2) == 0

            @pl.when((gz < to) & alike)
            def _():
                act(lift(to, gy, 0))

            for end, first in ((ny - 1, 0), (1, ny // 2)):

                @pl.when((gz < to) & jnp.logical_not(alike) & (gy == end))
                def _():
                    for n in range(ny // 2):
                        act(lift(to, first + n, n))

    lifts(lambda x: x.start())
    for n in range(nz - 1):

        @pl.when(n < gz)
        def _():
            copy(SM.at[1], SC.at[n], sc_s.at[0, 0], sc_r.at[n], {"gz": gz}).wait_recv()

    below = jnp.zeros_like(planes)
    for n in range(nz - 1):
        below = below + jnp.where(n < gz, SC[n], 0.0)
    cells = 1.0 / (rows * nx * 128 * ny)
    mean = jnp.broadcast_to(planes * cells, (8, 128))
    lane = lax.broadcasted_iota(jnp.int32, (8, 128), 1)
    upto = mean
    for n in (1, 2, 4, 8, 16):
        upto = upto + jnp.where(lane >= n, pltpu.roll(upto, n, 1), 0.0)
    rank = (lane + (gz * 4 * ny + 1)).astype(jnp.float32)
    pm_ref[...] = mean
    rm_ref[...] = (upto + jnp.sum(below, axis=(0, 1), keepdims=True) * cells) / rank
    lifts(lambda x: x.wait_send())

    for d in range(ny):
        whole = o_ref.at[pl.ds(0, 4)]
        if d == 0:
            pltpu.make_async_copy(N.at[:, 0, pl.ds(0, rows), :], whole, orem.at[0]).wait()
        else:
            end = copy(
                N.at[:, 0, pl.ds(0, rows), :], whole, osem.at[d], orem.at[d],
                {"gy": lax.rem(gy + d, ny)},
            )
            end.wait()
    for d in range(1, nx):
        to = {"gx": lax.rem(gx + d, nx)}
        at = pl.ds(8, rows)
        copy(E.at[1, :, at, :], E.at[1, :, at, :], xsE.at[d], xrE.at[0, d, 0], to).wait_send()
        copy(F.at[:, 1, :, at, :], F.at[:, 1, :, at, :], xsF.at[d], xrF.at[0, d, 0], to).wait_send()
        for side in (0, 1):

            @pl.when(has_edge(lax.rem(gx + d, nx), side))
            def _():
                for x in x_edge(d, side):
                    x.wait_send()
    for side in (0, 1):

        @pl.when(has_edge(gx, side))
        def _():
            x_half(side).wait_send()

    for way in (0, 1):
        for x in z_window(way, pl.ds(8, rows + 1), 0):
            x.wait_send()
        h_window(way, pl.ds(7, rows), 0).wait_send()


def per_device(energy, flow):
    nx, ny, nz = (lax.axis_size(a) for a in ("gx", "gy", "gz"))
    e = energy.reshape(32, 8, 8, 128).transpose(0, 2, 1, 3)
    f = flow.reshape(4, 32, 8, 8, 128).transpose(0, 1, 3, 2, 4)
    vmem = pl.BlockSpec(memory_space=pltpu.VMEM)
    hbm = pl.BlockSpec(memory_space=pl.ANY)
    f32 = jnp.float32
    dma = pltpu.SemaphoreType.DMA
    result, mean, running = pl.pallas_call(
        functools.partial(kernel, nx, ny, nz),
        out_shape=(
            jax.ShapeDtypeStruct((32, 64, 128), f32),
            jax.ShapeDtypeStruct((8, 128), f32),
            jax.ShapeDtypeStruct((8, 128), f32),
        ),
        in_specs=[hbm, hbm],
        out_specs=(hbm, vmem, vmem),
        scratch_shapes=[
            pltpu.VMEM((6, 8, 80, 128), f32),
            pltpu.VMEM((4, 6, 8, 80, 128), f32),
            pltpu.VMEM((6, 8, 80, 128), f32),
            pltpu.VMEM((4, 8, 64, 128), f32),
            pltpu.VMEM((4, 8, 128), f32),
            pltpu.VMEM((32, 1, 128), f32),
            pltpu.VMEM((8, 1, 128), f32),
            pltpu.VMEM((2, 1, 128), f32),
            dma((4,)), dma((4,)), dma((2, 4, 8)), dma((2, 4, 8)),
            dma((4, 2)), dma((4, 2)), dma((4, 2)), dma((4, 2)), dma((2,)), dma((2,)),
            dma((2,)), dma((2,)), dma((2,)), dma((2, 9)), dma((2, 9)), dma((2, 9)),
            dma((8,)), dma((8,)),
            dma((32,)), dma((32,)), dma((8, 4)), dma((8,)),
            pltpu.SemaphoreType.REGULAR((8,)),
        ],
        compiler_params=pltpu.CompilerParams(
            collective_id=0, has_side_effects=True, vmem_limit_bytes=55_000_000
        ),
        name="two_steps",
    )(e, f)
    return result, mean[0, :32], running[0, :32]


def solution(mesh):
    placed = (P(("gz", "gy", "gx"), None, None), P(None, ("gz", "gy", "gx"), None, None))
    return jax.shard_map(
        per_device,
        mesh=mesh,
        in_specs=placed,
        out_specs=(P("gz", "gx", "gy"), P("gz"), P("gz")),
        check_vma=False,
    )
```

```python
import functools

import jax
import jax.numpy as jnp
from jax import lax
from jax.experimental import pallas as pl
from jax.experimental.pallas import tpu as pltpu
from jax.sharding import PartitionSpec as P

MESH = pl.DeviceIdType.MESH
AHEAD = 3


def change_of(X, p, xi, F, fi):
    here = X[p, :, pl.ds(xi, 8), :]
    kappa = F[3, p, :, pl.ds(fi, 8), :]
    lane = lax.broadcasted_iota(jnp.int32, here.shape, 2)
    none = jnp.zeros_like(here[:1])

    def right(v):
        r = pltpu.roll(v, 127, 2)
        return jnp.where(lane == 127, jnp.concatenate([r[1:], none], 0), r)

    def left(v):
        r = pltpu.roll(v, 1, 2)
        return jnp.where(lane == 0, jnp.concatenate([none, r[:-1]], 0), r)

    sides = (
        (
            0,
            X[p + 1, :, pl.ds(xi, 8), :],
            F[3, p + 1, :, pl.ds(fi, 8), :],
            X[p - 1, :, pl.ds(xi, 8), :],
            F[3, p - 1, :, pl.ds(fi, 8), :],
        ),
        (
            1,
            X[p, :, pl.ds(xi + 1, 8), :],
            F[3, p, :, pl.ds(fi + 1, 8), :],
            X[p, :, pl.ds(xi - 1, 8), :],
            F[3, p, :, pl.ds(fi - 1, 8), :],
        ),
        (2, right(here), right(kappa), left(here), left(kappa)),
    )
    change = jnp.zeros_like(here)
    for axis, upper, kappa_upper, lower, kappa_lower in sides:
        speed = F[axis, p, :, pl.ds(fi, 8), :]
        change = (
            change
            + (0.5 * (kappa + kappa_upper) - jnp.minimum(speed, 0.0)) * (upper - here)
            - (0.5 * (kappa + kappa_lower) + jnp.maximum(speed, 0.0)) * (here - lower)
        )
    return here + change


def kernel(
    nx, ny, nz, e_ref, f_ref, o_ref, pm_ref, rm_ref, E, F, H, N, acc, SA, SC, SM,
    xsE, xsK, xsU, xrE, xrK, xrU, gsE, gsK, grE, grK, xsH, xrH, zsE, zsK, zsH, zrE, zrK, zrH,
    osem, orem, sa_s, sa_r, sc_s, sc_r, tok,
):
    gx, gy, gz = (lax.axis_index(a) for a in ("gx", "gy", "gz"))
    ring = ny * nz
    m = gz * ny + gy
    up, down = lax.rem(m + 1, ring), lax.rem(m + ring - 1, ring)
    chain = tuple({"gy": lax.rem(n, ny), "gz": n // ny} for n in (up, down))
    rounds = (ring - 1).bit_length() - 1
    rows = 64
    tiles = rows // 8

    bar = pltpu.get_barrier_semaphore()
    for d in range(1, nx):
        pl.semaphore_signal(
            bar, inc=1, device_id={"gx": lax.rem(gx + d, nx)}, device_id_type=MESH
        )
    for to in chain:
        pl.semaphore_signal(bar, inc=1, device_id=to, device_id_type=MESH)

    def copy(src, dst, send, recv, to):
        return pltpu.make_async_remote_copy(
            src_ref=src, dst_ref=dst, send_sem=send, recv_sem=recv, device_id=to,
            device_id_type=MESH,
        )

    def x_rows(kind, d, part, c):
        t = lax.rem(gx + d, nx)
        inside = (pl.ds(0, 2), pl.ds(2, 6))[part]
        at = pl.ds(8 + 8 * c + 2 * part, (2, 6)[part])
        parts = (
            (e_ref.at[t * tiles + c, :, inside, :], E.at[1 + gx, :, at, :], xsE, xrE),
            (f_ref.at[3, t * tiles + c, :, inside, :], F.at[3, 1 + gx, :, at, :], xsK, xrK),
            (
                f_ref.at[pl.ds(0, 3), t * tiles + c, :, inside, :],
                F.at[pl.ds(0, 3), 1 + gx, :, at, :],
                xsU,
                xrU,
            ),
        )
        parts = (parts[:2], parts[2:])[kind]
        if d == 0:
            return [pltpu.make_async_copy(a, b, r.at[part, 0, c]) for a, b, s, r in parts]
        return [copy(a, b, s.at[d], r.at[part, d, c], {"gx": t}) for a, b, s, r in parts]

    def x_edge(d, side):
        t = lax.rem(gx + d, nx)
        if side == 0:
            tile, row, at = lax.max(t * tiles - 1, 0), pl.ds(7, 1), pl.ds(7, 1)
        else:
            tile, row, at = lax.min((t + 1) * tiles, nx * tiles - 1), pl.ds(0, 1), pl.ds(8 + rows, 1)
        parts = (
            (e_ref.at[tile, :, row, :], E.at[1 + gx, :, at, :], gsE, grE),
            (f_ref.at[3, tile, :, row, :], F.at[3, 1 + gx, :, at, :], gsK, grK),
        )
        if d == 0:
            return [pltpu.make_async_copy(a, b, r.at[0, side]) for a, b, s, r in parts]
        return [copy(a, b, s.at[d, side], r.at[d, side], {"gx": t}) for a, b, s, r in parts]

    def x_half(side):
        src, dst = ((7, 71), (70, 6))[side]
        return copy(
            H.at[pl.ds(1, 4), :, pl.ds(src, 1), :], H.at[pl.ds(1, 4), :, pl.ds(dst, 1), :],
            xsH.at[side], xrH.at[side], {"gx": lax.rem(gx + (nx - 1, 1)[side], nx)},
        )

    def has_edge(g, side):
        return g > 0 if side == 0 else g < nx - 1

    def start_rows(kind, part, c):
        for d in range(nx):
            for x in x_rows(kind, d, part, c):
                x.start()

    def start_tile(kind, c):
        start_rows(kind, 1, c)

        @pl.when(c < tiles - 1)
        def _():
            start_rows(kind, 0, lax.min(c + 1, tiles - 1))

    def start_edges(side):
        for d in range(nx):

            @pl.when(has_edge(lax.rem(gx + d, nx), side))
            def _():
                for x in x_edge(d, side):
                    x.start()

    def z_window(way, at, c):
        src, dst = ((4, 0), (1, 5))[way]
        return (
            copy(E.at[src, :, at, :], E.at[dst, :, at, :], zsE.at[way], zrE.at[way, c], chain[way]),
            copy(
                F.at[3, src, :, at, :], F.at[3, dst, :, at, :], zsK.at[way], zrK.at[way, c],
                chain[way],
            ),
        )

    def h_window(way, at, c):
        src, dst = ((4, 0), (1, 5))[way]
        return copy(
            H.at[src, :, at, :], H.at[dst, :, at, :], zsH.at[way], zrH.at[way, c], chain[way]
        )

    def out_window(d, at):
        t = lax.rem(gy + d, ny)
        return copy(
            N.at[:, t, at, :], o_ref.at[pl.ds(4 * gy, 4), at, :], osem.at[d], orem.at[d],
            {"gy": t},
        )

    def send_out(at):
        def one(d, _):
            out_window(d, at).start()
            return 0

        lax.fori_loop(1, ny, one, 0)
        pltpu.make_async_copy(
            N.at[:, gy, at, :], o_ref.at[pl.ds(4 * gy, 4), at, :], orem.at[0]
        ).start()

    def over(planes, work):
        def one(n, _):
            work(planes[0] + (planes[1] - planes[0]) * n)
            return 0

        lax.fori_loop(0, 2, one, 0)

    inner, outer = (2, 3), (1, 4)

    def half(c, planes, first=0, count=8):
        def plane(p):
            v = change_of(E, p, 8 * c + 9, F, 8 * c + 9)
            at = 8 * c + 8 + first if count < 8 else pl.multiple_of(8 * c + 8, 8)
            H[p, :, pl.ds(at, count), :] = v[:, first : first + count]

        over(planes, plane)

    def full(c, planes):
        def plane(p):
            v = change_of(H, p, 8 * c + 7, F, pl.multiple_of(8 * c + 8, 8))
            N[p - 1, :, pl.ds(pl.multiple_of(8 * c, 8), 8), :] = v
            acc[p - 1] += jnp.sum(v, axis=0)

        over(planes, plane)

    def wait_rows(kind, part, c):
        for d in range(nx):
            for x in x_rows(kind, d, part, c):
                x.wait() if d == 0 else x.wait_recv()

    def wait_tile(kind, c):
        wait_rows(kind, 1, c)

        @pl.when(c < tiles - 1)
        def _():
            wait_rows(kind, 0, lax.min(c + 1, tiles - 1))

    def wait_edges(side):
        @pl.when(has_edge(gx, side))
        def _():
            for d in range(nx):
                for x in x_edge(d, side):
                    x.wait() if d == 0 else x.wait_recv()

    def out_at(c):
        return pl.ds(pl.multiple_of(8 * c, 8), 8)

    acc[...] = jnp.zeros_like(acc)
    for side, at, half_at in ((0, 7, 6), (1, 8 + rows, 7 + rows)):

        @pl.when(jnp.logical_not(has_edge(gx, side)))
        def _():
            none = jnp.zeros((4, ny, 1, 128), jnp.float32)
            E[1:5, :, at : at + 1, :] = none
            F[3, 1:5, :, at : at + 1, :] = none
            H[1:5, :, half_at : half_at + 1, :] = none

    pl.semaphore_wait(bar, nx + 1)
    start_edges(0)
    start_rows(0, 0, 0)
    start_tile(0, 0)
    start_edges(1)
    start_rows(1, 0, 0)
    for c in range(1, AHEAD):
        start_tile(0, c)
        start_tile(1, c - 1)
    wait_edges(0)
    wait_rows(0, 0, 0)

    def greet(r):
        for n in (2**r, ring - 2**r):
            to = lax.rem(m + n, ring)
            pl.semaphore_signal(
                tok.at[r], inc=1, device_id={"gy": lax.rem(to, ny), "gz": to // ny},
                device_id_type=MESH,
            )

    def start_z(at, c):
        for way in (0, 1):
            for x in z_window(way, at, c):
                x.start()

    def wait_z(at, c):
        for way in (0, 1):
            for x in z_window(way, at, c):
                x.wait_recv()

    def start_h(at, c):
        for way in (0, 1):
            h_window(way, at, c).start()

    def wait_h(at, c):
        for way in (0, 1):
            h_window(way, at, c).wait_recv()

    def z_at(c):
        return pl.ds(8 * c + 9, 8)

    def h_at(c):
        return pl.ds(pl.multiple_of(8 * c + 8, 8), 8)

    z_first, h_first = pl.ds(8, 1), pl.ds(7, 1)
    last = tiles - 1
    h_last = pl.ds(8 * last + 8, 7)
    start_z(z_first, tiles)

    def step(c, _):
        @pl.when(c + AHEAD < tiles)
        def _():
            start_tile(0, c + AHEAD)

        @pl.when(c + AHEAD - 1 < tiles)
        def _():
            start_tile(1, c + AHEAD - 1)

        for r in range(rounds):

            @pl.when(c == r)
            def _():
                if r > 0:
                    pl.semaphore_wait(tok.at[r - 1], 2)
                greet(r)

        @pl.when(c == rounds)
        def _():
            pl.semaphore_wait(tok.at[rounds - 1], 2)

        @pl.when(c == last)
        def _():
            wait_edges(1)

        wait_tile(0, c)
        start_z(z_at(c), c)

        @pl.when(c == 1)
        def _():
            wait_rows(1, 0, 0)
            wait_z(z_first, tiles)
            half(-1, inner, 7, 1)
            half(-1, outer, 7, 1)
            start_h(h_first, tiles)

            @pl.when(has_edge(gx, 0))
            def _():
                x_half(0).start()

        @pl.when(c >= 1)
        def _():
            wait_tile(1, c - 1)
            half(c - 1, inner)
            wait_z(z_at(c - 1), c - 1)
            half(c - 1, outer)
            start_h(h_at(c - 1), c - 1)

        @pl.when(c == 2)
        def _():
            wait_h(h_first, tiles)

        @pl.when(c == 2)
        def _():
            wait_h(h_at(0), 0)

        @pl.when(c >= 3)
        def _():
            full(c - 2, inner)
            wait_h(h_at(c - 2), c - 2)
            full(c - 2, outer)

        @pl.when(c == 4)
        def _():
            send_out(out_at(1))

        @pl.when(c >= 4)
        def _():
            send_out(out_at(c - 2))

        return 0

    lax.fori_loop(0, tiles, step, 0)
    wait_z(z_at(last), last)
    wait_rows(1, 1, last)
    half(last, outer, 0, 7)
    start_h(h_last, last)
    half(last, inner, 0, 7)

    @pl.when(has_edge(gx, 1))
    def _():
        x_half(1).start()

    full(last - 1, inner)
    wait_h(h_at(last - 1), last - 1)
    full(last - 1, outer)
    send_out(out_at(last - 1))

    @pl.when(has_edge(gx, 1))
    def _():
        x_half(0).wait_recv()

    full(last, inner)
    wait_h(h_last, last)
    full(last, outer)

    @pl.when(has_edge(gx, 0))
    def _():
        x_half(1).wait_recv()

    full(0, inner)
    full(0, outer)

    lane = lax.broadcasted_iota(jnp.int32, (1, 128), 1)
    part = jnp.zeros((1, 128), jnp.float32)
    for p in range(4):
        part = part + jnp.where(
            lane == 4 * gy + p, jnp.sum(acc[p], axis=(0, 1), keepdims=True), 0.0
        )
    SM[0] = part
    SA[gx * ny + gy] = part

    def group_row(n):
        to = lax.rem(gx * ny + gy + n, nx * ny)
        return copy(
            SM.at[0], SA.at[gx * ny + gy], sa_s.at[n], sa_r.at[n],
            {"gx": to // ny, "gy": lax.rem(to, ny)},
        )

    def start_row(n, _):
        group_row(n).start()
        return 0

    def wait_row(n, _):
        group_row(n).wait()
        return 0

    lax.fori_loop(1, nx * ny, start_row, 0)
    send_out(out_at(last))
    send_out(out_at(0))
    lax.fori_loop(1, nx * ny, wait_row, 0)
    planes = jnp.sum(SA[...], axis=0)
    SM[1] = planes

    def lift(to_z, to_y, slot):
        return copy(
            SM.at[1], SC.at[gz], sc_s.at[to_z, slot], sc_r.at[gz], {"gy": to_y, "gz": to_z}
        )

    def lifts(act):
        for to in range(1, nz):
            alike = lax.rem(gz + to, 2) == 0

            @pl.when((gz < to) & alike)
            def _():
                act(lift(to, gy, 0))

            for end, first in ((ny - 1, 0), (1, ny // 2)):

                @pl.when((gz < to) & jnp.logical_not(alike) & (gy == end))
                def _():
                    for n in range(ny // 2):
                        act(lift(to, first + n, n))

    lifts(lambda x: x.start())
    for n in range(nz - 1):

        @pl.when(n < gz)
        def _():
            copy(SM.at[1], SC.at[n], sc_s.at[0, 0], sc_r.at[n], {"gz": gz}).wait_recv()

    below = jnp.zeros_like(planes)
    for n in range(nz - 1):
        below = below + jnp.where(n < gz, SC[n], 0.0)
    cells = 1.0 / (rows * nx * 128 * ny)
    mean = jnp.broadcast_to(planes * cells, (8, 128))
    lane = lax.broadcasted_iota(jnp.int32, (8, 128), 1)
    upto = mean
    for n in (1, 2, 4, 8, 16):
        upto = upto + jnp.where(lane >= n, pltpu.roll(upto, n, 1), 0.0)
    rank = (lane + (gz * 4 * ny + 1)).astype(jnp.float32)
    pm_ref[...] = mean
    rm_ref[...] = (upto + jnp.sum(below, axis=(0, 1), keepdims=True) * cells) / rank
    lifts(lambda x: x.wait_send())

    for d in range(ny):
        whole = o_ref.at[pl.ds(0, 4)]
        if d == 0:
            pltpu.make_async_copy(N.at[:, 0, pl.ds(0, rows), :], whole, orem.at[0]).wait()
        else:
            end = copy(
                N.at[:, 0, pl.ds(0, rows), :], whole, osem.at[d], orem.at[d],
                {"gy": lax.rem(gy + d, ny)},
            )
            end.wait()
    for d in range(1, nx):
        to = {"gx": lax.rem(gx + d, nx)}
        at = pl.ds(8, rows)
        copy(E.at[1, :, at, :], E.at[1, :, at, :], xsE.at[d], xrE.at[0, d, 0], to).wait_send()
        copy(E.at[1, :, at, :], E.at[1, :, at, :], xsK.at[d], xrK.at[0, d, 0], to).wait_send()
        three = F.at[pl.ds(0, 3), 1, :, at, :]
        copy(three, three, xsU.at[d], xrU.at[0, d, 0], to).wait_send()
        for side in (0, 1):

            @pl.when(has_edge(lax.rem(gx + d, nx), side))
            def _():
                for x in x_edge(d, side):
                    x.wait_send()
    for side in (0, 1):

        @pl.when(has_edge(gx, side))
        def _():
            x_half(side).wait_send()

    for way in (0, 1):
        for x in z_window(way, pl.ds(8, rows + 1), 0):
            x.wait_send()
        h_window(way, pl.ds(7, rows), 0).wait_send()


def per_device(energy, flow):
    nx, ny, nz = (lax.axis_size(a) for a in ("gx", "gy", "gz"))
    e = energy.reshape(32, 8, 8, 128).transpose(0, 2, 1, 3)
    f = flow.reshape(4, 32, 8, 8, 128).transpose(0, 1, 3, 2, 4)
    vmem = pl.BlockSpec(memory_space=pltpu.VMEM)
    hbm = pl.BlockSpec(memory_space=pl.ANY)
    f32 = jnp.float32
    dma = pltpu.SemaphoreType.DMA
    result, mean, running = pl.pallas_call(
        functools.partial(kernel, nx, ny, nz),
        out_shape=(
            jax.ShapeDtypeStruct((32, 64, 128), f32),
            jax.ShapeDtypeStruct((8, 128), f32),
            jax.ShapeDtypeStruct((8, 128), f32),
        ),
        in_specs=[hbm, hbm],
        out_specs=(hbm, vmem, vmem),
        scratch_shapes=[
            pltpu.VMEM((6, 8, 80, 128), f32),
            pltpu.VMEM((4, 6, 8, 80, 128), f32),
            pltpu.VMEM((6, 8, 80, 128), f32),
            pltpu.VMEM((4, 8, 64, 128), f32),
            pltpu.VMEM((4, 8, 128), f32),
            pltpu.VMEM((32, 1, 128), f32),
            pltpu.VMEM((8, 1, 128), f32),
            pltpu.VMEM((2, 1, 128), f32),
            dma((4,)), dma((4,)), dma((4,)), dma((2, 4, 8)), dma((2, 4, 8)), dma((2, 4, 8)),
            dma((4, 2)), dma((4, 2)), dma((4, 2)), dma((4, 2)), dma((2,)), dma((2,)),
            dma((2,)), dma((2,)), dma((2,)), dma((2, 9)), dma((2, 9)), dma((2, 9)),
            dma((8,)), dma((8,)),
            dma((32,)), dma((32,)), dma((8, 4)), dma((8,)),
            pltpu.SemaphoreType.REGULAR((8,)),
        ],
        compiler_params=pltpu.CompilerParams(
            collective_id=0, has_side_effects=True, vmem_limit_bytes=55_000_000
        ),
        name="two_steps",
    )(e, f)
    return result, mean[0, :32], running[0, :32]


def solution(mesh):
    placed = (P(("gz", "gy", "gx"), None, None), P(None, ("gz", "gy", "gx"), None, None))
    return jax.shard_map(
        per_device,
        mesh=mesh,
        in_specs=placed,
        out_specs=(P("gz", "gx", "gy"), P("gz"), P("gz")),
        check_vma=False,
    )
```

```python
import functools

import jax
import jax.numpy as jnp
from jax import lax
from jax.experimental import pallas as pl
from jax.experimental.pallas import tpu as pltpu
from jax.sharding import PartitionSpec as P

MESH = pl.DeviceIdType.MESH
AHEAD = 3


def change_of(X, p, xi, F, fi):
    here = X[p, :, pl.ds(xi, 8), :]
    kappa = F[3, p, :, pl.ds(fi, 8), :]
    lane = lax.broadcasted_iota(jnp.int32, here.shape, 2)
    none = jnp.zeros_like(here[:1])

    def right(v):
        r = pltpu.roll(v, 127, 2)
        return jnp.where(lane == 127, jnp.concatenate([r[1:], none], 0), r)

    def left(v):
        r = pltpu.roll(v, 1, 2)
        return jnp.where(lane == 0, jnp.concatenate([none, r[:-1]], 0), r)

    sides = (
        (
            0,
            X[p + 1, :, pl.ds(xi, 8), :],
            F[3, p + 1, :, pl.ds(fi, 8), :],
            X[p - 1, :, pl.ds(xi, 8), :],
            F[3, p - 1, :, pl.ds(fi, 8), :],
        ),
        (
            1,
            X[p, :, pl.ds(xi + 1, 8), :],
            F[3, p, :, pl.ds(fi + 1, 8), :],
            X[p, :, pl.ds(xi - 1, 8), :],
            F[3, p, :, pl.ds(fi - 1, 8), :],
        ),
        (2, right(here), right(kappa), left(here), left(kappa)),
    )
    change = jnp.zeros_like(here)
    for axis, upper, kappa_upper, lower, kappa_lower in sides:
        speed = F[axis, p, :, pl.ds(fi, 8), :]
        change = (
            change
            + (0.5 * (kappa + kappa_upper) - jnp.minimum(speed, 0.0)) * (upper - here)
            - (0.5 * (kappa + kappa_lower) + jnp.maximum(speed, 0.0)) * (here - lower)
        )
    return here + change


def kernel(
    nx, ny, nz, e_ref, f_ref, o_ref, pm_ref, rm_ref, E, F, H, N, below_row, acc, SA, SC, SM,
    xsE, xsK, xsU, xrE, xrK, xrU, gsE, gsK, grE, grK, xsH, xrH, zsE, zsK, zsH, zrE, zrK, zrH,
    osem, orem, sa_s, sa_r, sc_s, sc_r, tok,
):
    gx, gy, gz = (lax.axis_index(a) for a in ("gx", "gy", "gz"))
    ring = ny * nz
    m = gz * ny + gy
    up, down = lax.rem(m + 1, ring), lax.rem(m + ring - 1, ring)
    chain = tuple({"gy": lax.rem(n, ny), "gz": n // ny} for n in (up, down))
    rounds = (ring - 1).bit_length() - 1
    rows = 64
    tiles = rows // 8

    bar = pltpu.get_barrier_semaphore()
    for d in range(1, nx):
        pl.semaphore_signal(
            bar, inc=1, device_id={"gx": lax.rem(gx + d, nx)}, device_id_type=MESH
        )
    for to in chain:
        pl.semaphore_signal(bar, inc=1, device_id=to, device_id_type=MESH)

    def copy(src, dst, send, recv, to):
        return pltpu.make_async_remote_copy(
            src_ref=src, dst_ref=dst, send_sem=send, recv_sem=recv, device_id=to,
            device_id_type=MESH,
        )

    def x_rows(kind, d, part, c):
        t = lax.rem(gx + d, nx)
        inside = (pl.ds(0, 2), pl.ds(2, 6))[part]
        at = pl.ds(8 + 8 * c + 2 * part, (2, 6)[part])
        parts = (
            (e_ref.at[t * tiles + c, :, inside, :], E.at[1 + gx, :, at, :], xsE, xrE),
            (f_ref.at[3, t * tiles + c, :, inside, :], F.at[3, 1 + gx, :, at, :], xsK, xrK),
            (
                f_ref.at[pl.ds(0, 3), t * tiles + c, :, inside, :],
                F.at[pl.ds(0, 3), 1 + gx, :, at, :],
                xsU,
                xrU,
            ),
        )
        parts = (parts[:2], parts[2:])[kind]
        if d == 0:
            return [pltpu.make_async_copy(a, b, r.at[part, 0, c]) for a, b, s, r in parts]
        return [copy(a, b, s.at[d], r.at[part, d, c], {"gx": t}) for a, b, s, r in parts]

    def x_edge(d, side):
        t = lax.rem(gx + d, nx)
        if side == 0:
            tile, row, at = lax.max(t * tiles - 1, 0), pl.ds(7, 1), pl.ds(7, 1)
        else:
            tile, row, at = lax.min((t + 1) * tiles, nx * tiles - 1), pl.ds(0, 1), pl.ds(8 + rows, 1)
        parts = (
            (e_ref.at[tile, :, row, :], E.at[1 + gx, :, at, :], gsE, grE),
            (f_ref.at[3, tile, :, row, :], F.at[3, 1 + gx, :, at, :], gsK, grK),
        )
        if d == 0:
            return [pltpu.make_async_copy(a, b, r.at[0, side]) for a, b, s, r in parts]
        return [copy(a, b, s.at[d, side], r.at[d, side], {"gx": t}) for a, b, s, r in parts]

    def x_half(side):
        src = H.at[pl.ds(1, 4), :, pl.ds((7, 70)[side], 1), :]
        return copy(
            src, below_row if side else H.at[pl.ds(1, 4), :, pl.ds(71, 1), :],
            xsH.at[side], xrH.at[side], {"gx": lax.rem(gx + (nx - 1, 1)[side], nx)},
        )

    def has_edge(g, side):
        return g > 0 if side == 0 else g < nx - 1

    def start_rows(kind, part, c):
        for d in range(nx):
            for x in x_rows(kind, d, part, c):
                x.start()

    def start_tile(kind, c):
        start_rows(kind, 1, c)

        @pl.when(c < tiles - 1)
        def _():
            start_rows(kind, 0, lax.min(c + 1, tiles - 1))

    def start_edges(side):
        for d in range(nx):

            @pl.when(has_edge(lax.rem(gx + d, nx), side))
            def _():
                for x in x_edge(d, side):
                    x.start()

    def z_window(way, at, c):
        src, dst = ((4, 0), (1, 5))[way]
        return (
            copy(E.at[src, :, at, :], E.at[dst, :, at, :], zsE.at[way], zrE.at[way, c], chain[way]),
            copy(
                F.at[3, src, :, at, :], F.at[3, dst, :, at, :], zsK.at[way], zrK.at[way, c],
                chain[way],
            ),
        )

    def h_window(way, at, c):
        src, dst = ((4, 0), (1, 5))[way]
        return copy(
            H.at[src, :, at, :], H.at[dst, :, at, :], zsH.at[way], zrH.at[way, c], chain[way]
        )

    def out_window(d, at):
        t = lax.rem(gy + d, ny)
        return copy(
            N.at[:, t, at, :], o_ref.at[pl.ds(4 * gy, 4), at, :], osem.at[d], orem.at[d],
            {"gy": t},
        )

    def send_out(at):
        def one(d, _):
            out_window(d, at).start()
            return 0

        lax.fori_loop(1, ny, one, 0)
        pltpu.make_async_copy(
            N.at[:, gy, at, :], o_ref.at[pl.ds(4 * gy, 4), at, :], orem.at[0]
        ).start()

    def over(planes, work):
        def one(n, _):
            work(planes[0] + (planes[1] - planes[0]) * n)
            return 0

        lax.fori_loop(0, 2, one, 0)

    inner, outer = (2, 3), (1, 4)

    def half(c, planes, first=0, count=8):
        def plane(p):
            v = change_of(E, p, 8 * c + 9, F, 8 * c + 9)
            at = 8 * c + 8 + first if count < 8 else pl.multiple_of(8 * c + 8, 8)
            H[p, :, pl.ds(at, count), :] = v[:, first : first + count]

        over(planes, plane)

    def full(c, planes, first=0, count=8):
        def plane(p):
            v = change_of(H, p, 8 * c + 7, F, pl.multiple_of(8 * c + 8, 8))
            if count < 8:
                N[p - 1, :, pl.ds(8 * c + first, count), :] = v[:, first : first + count]
                row = lax.broadcasted_iota(jnp.int32, v.shape, 1)
                v = jnp.where((row >= first) & (row < first + count), v, 0.0)
            else:
                N[p - 1, :, pl.ds(pl.multiple_of(8 * c, 8), 8), :] = v
            acc[p - 1] += jnp.sum(v, axis=0)

        over(planes, plane)

    def wait_rows(kind, part, c):
        for d in range(nx):
            for x in x_rows(kind, d, part, c):
                x.wait() if d == 0 else x.wait_recv()

    def wait_tile(kind, c):
        wait_rows(kind, 1, c)

        @pl.when(c < tiles - 1)
        def _():
            wait_rows(kind, 0, lax.min(c + 1, tiles - 1))

    def wait_edges(side):
        @pl.when(has_edge(gx, side))
        def _():
            for d in range(nx):
                for x in x_edge(d, side):
                    x.wait() if d == 0 else x.wait_recv()

    def out_at(c):
        return pl.ds(pl.multiple_of(8 * c, 8), 8)

    acc[...] = jnp.zeros_like(acc)
    for side, at, half_at in ((0, 7, 6), (1, 8 + rows, 7 + rows)):

        @pl.when(jnp.logical_not(has_edge(gx, side)))
        def _():
            none = jnp.zeros((4, ny, 1, 128), jnp.float32)
            E[1:5, :, at : at + 1, :] = none
            F[3, 1:5, :, at : at + 1, :] = none
            H[1:5, :, half_at : half_at + 1, :] = none

    pl.semaphore_wait(bar, nx + 1)
    start_edges(0)
    start_rows(0, 0, 0)
    start_tile(0, 0)
    start_edges(1)
    start_rows(1, 0, 0)
    for c in range(1, AHEAD):
        start_tile(0, c)
        start_tile(1, c - 1)
    wait_edges(0)
    wait_rows(0, 0, 0)

    def greet(r):
        for n in (2**r, ring - 2**r):
            to = lax.rem(m + n, ring)
            pl.semaphore_signal(
                tok.at[r], inc=1, device_id={"gy": lax.rem(to, ny), "gz": to // ny},
                device_id_type=MESH,
            )

    def start_z(at, c):
        for way in (0, 1):
            for x in z_window(way, at, c):
                x.start()

    def wait_z(at, c):
        for way in (0, 1):
            for x in z_window(way, at, c):
                x.wait_recv()

    def start_h(at, c):
        for way in (0, 1):
            h_window(way, at, c).start()

    def wait_h(at, c):
        for way in (0, 1):
            h_window(way, at, c).wait_recv()

    def z_at(c):
        return pl.ds(8 * c + 9, 8)

    def h_at(c):
        return pl.ds(pl.multiple_of(8 * c + 8, 8), 8)

    z_first, h_first = pl.ds(8, 1), pl.ds(7, 1)
    last = tiles - 1
    h_last = pl.ds(8 * last + 8, 7)
    start_z(z_first, tiles)

    def step(c, _):
        @pl.when(c + AHEAD < tiles)
        def _():
            start_tile(0, c + AHEAD)

        @pl.when(c + AHEAD - 1 < tiles)
        def _():
            start_tile(1, c + AHEAD - 1)

        for r in range(rounds):

            @pl.when(c == r)
            def _():
                if r > 0:
                    pl.semaphore_wait(tok.at[r - 1], 2)
                greet(r)

        @pl.when(c == rounds)
        def _():
            pl.semaphore_wait(tok.at[rounds - 1], 2)

        @pl.when(c == last)
        def _():
            wait_edges(1)

        wait_tile(0, c)
        start_z(z_at(c), c)

        @pl.when(c == 1)
        def _():
            wait_rows(1, 0, 0)
            wait_z(z_first, tiles)
            half(-1, inner, 7, 1)
            half(-1, outer, 7, 1)
            start_h(h_first, tiles)

            @pl.when(has_edge(gx, 0))
            def _():
                x_half(0).start()

        @pl.when(c >= 1)
        def _():
            wait_tile(1, c - 1)
            half(c - 1, inner)
            wait_z(z_at(c - 1), c - 1)
            half(c - 1, outer)
            start_h(h_at(c - 1), c - 1)

        @pl.when(c == 2)
        def _():
            full(0, inner, 1, 7)
            wait_h(h_first, tiles)
            wait_h(h_at(0), 0)
            full(0, outer, 1, 7)

        @pl.when(c >= 3)
        def _():
            full(c - 2, inner)
            wait_h(h_at(c - 2), c - 2)
            full(c - 2, outer)

        @pl.when(c == 4)
        def _():
            send_out(pl.ds(1, 7))
            send_out(out_at(1))

        @pl.when(c >= 4)
        def _():
            send_out(out_at(c - 2))

        return 0

    lax.fori_loop(0, tiles, step, 0)
    wait_z(z_at(last), last)
    wait_rows(1, 1, last)
    half(last, outer, 0, 7)
    start_h(h_last, last)
    half(last, inner, 0, 7)

    @pl.when(has_edge(gx, 1))
    def _():
        x_half(1).start()

    full(last - 1, inner)
    wait_h(h_at(last - 1), last - 1)
    full(last - 1, outer)

    @pl.when(has_edge(gx, 1))
    def _():
        x_half(0).wait_recv()

    full(last, inner)
    wait_h(h_last, last)
    full(last, outer)

    @pl.when(has_edge(gx, 0))
    def _():
        x_half(1).wait_recv()
        H[1:5, :, 6:7, :] = below_row[...]

    full(0, inner, 0, 1)
    full(0, outer, 0, 1)

    lane = lax.broadcasted_iota(jnp.int32, (1, 128), 1)
    part = jnp.zeros((1, 128), jnp.float32)
    for p in range(4):
        part = part + jnp.where(
            lane == 4 * gy + p, jnp.sum(acc[p], axis=(0, 1), keepdims=True), 0.0
        )
    SM[0] = part
    SA[gx * ny + gy] = part

    def group_row(n):
        to = lax.rem(gx * ny + gy + n, nx * ny)
        return copy(
            SM.at[0], SA.at[gx * ny + gy], sa_s.at[n], sa_r.at[n],
            {"gx": to // ny, "gy": lax.rem(to, ny)},
        )

    def start_row(n, _):
        group_row(n).start()
        return 0

    def wait_row(n, _):
        group_row(n).wait()
        return 0

    lax.fori_loop(1, nx * ny, start_row, 0)
    send_out(out_at(last - 1))
    send_out(out_at(last))
    send_out(pl.ds(0, 1))
    lax.fori_loop(1, nx * ny, wait_row, 0)
    planes = jnp.sum(SA[...], axis=0)
    SM[1] = planes

    def lift(to_z, to_y, slot):
        return copy(
            SM.at[1], SC.at[gz], sc_s.at[to_z, slot], sc_r.at[gz], {"gy": to_y, "gz": to_z}
        )

    def lifts(act):
        for to in range(1, nz):
            alike = lax.rem(gz + to, 2) == 0

            @pl.when((gz < to) & alike)
            def _():
                act(lift(to, gy, 0))

            for end, first in ((ny - 1, 0), (1, ny // 2)):

                @pl.when((gz < to) & jnp.logical_not(alike) & (gy == end))
                def _():
                    for n in range(ny // 2):
                        act(lift(to, first + n, n))

    lifts(lambda x: x.start())
    for n in range(nz - 1):

        @pl.when(n < gz)
        def _():
            copy(SM.at[1], SC.at[n], sc_s.at[0, 0], sc_r.at[n], {"gz": gz}).wait_recv()

    below = jnp.zeros_like(planes)
    for n in range(nz - 1):
        below = below + jnp.where(n < gz, SC[n], 0.0)
    cells = 1.0 / (rows * nx * 128 * ny)
    mean = jnp.broadcast_to(planes * cells, (8, 128))
    lane = lax.broadcasted_iota(jnp.int32, (8, 128), 1)
    upto = mean
    for n in (1, 2, 4, 8, 16):
        upto = upto + jnp.where(lane >= n, pltpu.roll(upto, n, 1), 0.0)
    rank = (lane + (gz * 4 * ny + 1)).astype(jnp.float32)
    pm_ref[...] = mean
    rm_ref[...] = (upto + jnp.sum(below, axis=(0, 1), keepdims=True) * cells) / rank
    lifts(lambda x: x.wait_send())

    for d in range(ny):
        whole = o_ref.at[pl.ds(0, 4)]
        if d == 0:
            pltpu.make_async_copy(N.at[:, 0, pl.ds(0, rows), :], whole, orem.at[0]).wait()
        else:
            end = copy(
                N.at[:, 0, pl.ds(0, rows), :], whole, osem.at[d], orem.at[d],
                {"gy": lax.rem(gy + d, ny)},
            )
            end.wait()
    for d in range(1, nx):
        to = {"gx": lax.rem(gx + d, nx)}
        at = pl.ds(8, rows)
        copy(E.at[1, :, at, :], E.at[1, :, at, :], xsE.at[d], xrE.at[0, d, 0], to).wait_send()
        copy(E.at[1, :, at, :], E.at[1, :, at, :], xsK.at[d], xrK.at[0, d, 0], to).wait_send()
        three = F.at[pl.ds(0, 3), 1, :, at, :]
        copy(three, three, xsU.at[d], xrU.at[0, d, 0], to).wait_send()
        for side in (0, 1):

            @pl.when(has_edge(lax.rem(gx + d, nx), side))
            def _():
                for x in x_edge(d, side):
                    x.wait_send()
    for side in (0, 1):

        @pl.when(has_edge(gx, side))
        def _():
            x_half(side).wait_send()

    for way in (0, 1):
        for x in z_window(way, pl.ds(8, rows + 1), 0):
            x.wait_send()
        h_window(way, pl.ds(7, rows), 0).wait_send()


def per_device(energy, flow):
    nx, ny, nz = (lax.axis_size(a) for a in ("gx", "gy", "gz"))
    e = energy.reshape(32, 8, 8, 128).transpose(0, 2, 1, 3)
    f = flow.reshape(4, 32, 8, 8, 128).transpose(0, 1, 3, 2, 4)
    vmem = pl.BlockSpec(memory_space=pltpu.VMEM)
    hbm = pl.BlockSpec(memory_space=pl.ANY)
    f32 = jnp.float32
    dma = pltpu.SemaphoreType.DMA
    result, mean, running = pl.pallas_call(
        functools.partial(kernel, nx, ny, nz),
        out_shape=(
            jax.ShapeDtypeStruct((32, 64, 128), f32),
            jax.ShapeDtypeStruct((8, 128), f32),
            jax.ShapeDtypeStruct((8, 128), f32),
        ),
        in_specs=[hbm, hbm],
        out_specs=(hbm, vmem, vmem),
        scratch_shapes=[
            pltpu.VMEM((6, 8, 80, 128), f32),
            pltpu.VMEM((4, 6, 8, 80, 128), f32),
            pltpu.VMEM((6, 8, 80, 128), f32),
            pltpu.VMEM((4, 8, 64, 128), f32),
            pltpu.VMEM((4, 8, 1, 128), f32),
            pltpu.VMEM((4, 8, 128), f32),
            pltpu.VMEM((32, 1, 128), f32),
            pltpu.VMEM((8, 1, 128), f32),
            pltpu.VMEM((2, 1, 128), f32),
            dma((4,)), dma((4,)), dma((4,)), dma((2, 4, 8)), dma((2, 4, 8)), dma((2, 4, 8)),
            dma((4, 2)), dma((4, 2)), dma((4, 2)), dma((4, 2)), dma((2,)), dma((2,)),
            dma((2,)), dma((2,)), dma((2,)), dma((2, 9)), dma((2, 9)), dma((2, 9)),
            dma((8,)), dma((8,)),
            dma((32,)), dma((32,)), dma((8, 4)), dma((8,)),
            pltpu.SemaphoreType.REGULAR((8,)),
        ],
        compiler_params=pltpu.CompilerParams(
            collective_id=0, has_side_effects=True, vmem_limit_bytes=55_000_000
        ),
        name="two_steps",
    )(e, f)
    return result, mean[0, :32], running[0, :32]


def solution(mesh):
    placed = (P(("gz", "gy", "gx"), None, None), P(None, ("gz", "gy", "gx"), None, None))
    return jax.shard_map(
        per_device,
        mesh=mesh,
        in_specs=placed,
        out_specs=(P("gz", "gx", "gy"), P("gz"), P("gz")),
        check_vma=False,
    )
```

```python
import functools

import jax
import jax.numpy as jnp
from jax import lax
from jax.experimental import pallas as pl
from jax.experimental.pallas import tpu as pltpu
from jax.sharding import PartitionSpec as P

MESH = pl.DeviceIdType.MESH
AHEAD = 3


def change_of(X, p, xi, F, fi):
    here = X[p, :, pl.ds(xi, 8), :]
    kappa = F[3, p, :, pl.ds(fi, 8), :]
    lane = lax.broadcasted_iota(jnp.int32, here.shape, 2)
    none = jnp.zeros_like(here[:1])

    def right(v):
        r = pltpu.roll(v, 127, 2)
        return jnp.where(lane == 127, jnp.concatenate([r[1:], none], 0), r)

    def left(v):
        r = pltpu.roll(v, 1, 2)
        return jnp.where(lane == 0, jnp.concatenate([none, r[:-1]], 0), r)

    sides = (
        (
            0,
            X[p + 1, :, pl.ds(xi, 8), :],
            F[3, p + 1, :, pl.ds(fi, 8), :],
            X[p - 1, :, pl.ds(xi, 8), :],
            F[3, p - 1, :, pl.ds(fi, 8), :],
        ),
        (
            1,
            X[p, :, pl.ds(xi + 1, 8), :],
            F[3, p, :, pl.ds(fi + 1, 8), :],
            X[p, :, pl.ds(xi - 1, 8), :],
            F[3, p, :, pl.ds(fi - 1, 8), :],
        ),
        (2, right(here), right(kappa), left(here), left(kappa)),
    )
    change = jnp.zeros_like(here)
    for axis, upper, kappa_upper, lower, kappa_lower in sides:
        speed = F[axis, p, :, pl.ds(fi, 8), :]
        change = (
            change
            + (0.5 * (kappa + kappa_upper) - jnp.minimum(speed, 0.0)) * (upper - here)
            - (0.5 * (kappa + kappa_lower) + jnp.maximum(speed, 0.0)) * (here - lower)
        )
    return here + change


def kernel(
    nx, ny, nz, e_ref, f_ref, o_ref, pm_ref, rm_ref, E, F, H, N, below_row, first_tile, acc, SA, SC, SM,
    xsE, xsK, xsU, xrE, xrK, xrU, gsE, gsK, grE, grK, xsH, xrH, zsE, zsK, zsH, zrE, zrK, zrH,
    osem, orem, fsem, sa_s, sa_r, sc_s, sc_r, tok,
):
    gx, gy, gz = (lax.axis_index(a) for a in ("gx", "gy", "gz"))
    ring = ny * nz
    m = gz * ny + gy
    up, down = lax.rem(m + 1, ring), lax.rem(m + ring - 1, ring)
    chain = tuple({"gy": lax.rem(n, ny), "gz": n // ny} for n in (up, down))
    rounds = (ring - 1).bit_length() - 1
    rows = 64
    tiles = rows // 8

    bar = pltpu.get_barrier_semaphore()
    for d in range(1, nx):
        pl.semaphore_signal(
            bar, inc=1, device_id={"gx": lax.rem(gx + d, nx)}, device_id_type=MESH
        )
    for to in chain:
        pl.semaphore_signal(bar, inc=1, device_id=to, device_id_type=MESH)

    def copy(src, dst, send, recv, to):
        return pltpu.make_async_remote_copy(
            src_ref=src, dst_ref=dst, send_sem=send, recv_sem=recv, device_id=to,
            device_id_type=MESH,
        )

    def x_rows(kind, d, part, c, staged=False):
        t = lax.rem(gx + d, nx)
        inside = (pl.ds(0, 2), pl.ds(2, 6))[part]
        at = pl.ds(8 + 8 * c + 2 * part, (2, 6)[part])
        e_from = first_tile.at[0, t] if staged else e_ref.at[t * tiles + c]
        k_from = first_tile.at[1, t] if staged else f_ref.at[3, t * tiles + c]
        parts = (
            (e_from.at[:, inside, :], E.at[1 + gx, :, at, :], xsE, xrE),
            (k_from.at[:, inside, :], F.at[3, 1 + gx, :, at, :], xsK, xrK),
            (
                f_ref.at[pl.ds(0, 3), t * tiles + c, :, inside, :],
                F.at[pl.ds(0, 3), 1 + gx, :, at, :],
                xsU,
                xrU,
            ),
        )
        parts = (parts[:2], parts[2:])[kind]
        if d == 0:
            return [pltpu.make_async_copy(a, b, r.at[part, 0, c]) for a, b, s, r in parts]
        return [copy(a, b, s.at[d], r.at[part, d, c], {"gx": t}) for a, b, s, r in parts]

    def x_edge(d, side):
        t = lax.rem(gx + d, nx)
        if side == 0:
            tile, row, at = lax.max(t * tiles - 1, 0), pl.ds(7, 1), pl.ds(7, 1)
        else:
            tile, row, at = lax.min((t + 1) * tiles, nx * tiles - 1), pl.ds(0, 1), pl.ds(8 + rows, 1)
        parts = (
            (e_ref.at[tile, :, row, :], E.at[1 + gx, :, at, :], gsE, grE),
            (f_ref.at[3, tile, :, row, :], F.at[3, 1 + gx, :, at, :], gsK, grK),
        )
        if d == 0:
            return [pltpu.make_async_copy(a, b, r.at[0, side]) for a, b, s, r in parts]
        return [copy(a, b, s.at[d, side], r.at[d, side], {"gx": t}) for a, b, s, r in parts]

    def x_half(side):
        src = H.at[pl.ds(1, 4), :, pl.ds((7, 70)[side], 1), :]
        return copy(
            src, below_row if side else H.at[pl.ds(1, 4), :, pl.ds(71, 1), :],
            xsH.at[side], xrH.at[side], {"gx": lax.rem(gx + (nx - 1, 1)[side], nx)},
        )

    def has_edge(g, side):
        return g > 0 if side == 0 else g < nx - 1

    def start_rows(kind, part, c, staged=False):
        for d in range(nx):
            for x in x_rows(kind, d, part, c, staged and d > 0):
                x.start()

    def start_tile(kind, c):
        start_rows(kind, 1, c)

        @pl.when(c < tiles - 1)
        def _():
            start_rows(kind, 0, lax.min(c + 1, tiles - 1))

    def start_edges(side):
        for d in range(nx):

            @pl.when(has_edge(lax.rem(gx + d, nx), side))
            def _():
                for x in x_edge(d, side):
                    x.start()

    def z_window(way, at, c):
        src, dst = ((4, 0), (1, 5))[way]
        return (
            copy(E.at[src, :, at, :], E.at[dst, :, at, :], zsE.at[way], zrE.at[way, c], chain[way]),
            copy(
                F.at[3, src, :, at, :], F.at[3, dst, :, at, :], zsK.at[way], zrK.at[way, c],
                chain[way],
            ),
        )

    def h_window(way, at, c):
        src, dst = ((4, 0), (1, 5))[way]
        return copy(
            H.at[src, :, at, :], H.at[dst, :, at, :], zsH.at[way], zrH.at[way, c], chain[way]
        )

    def out_window(d, at):
        t = lax.rem(gy + d, ny)
        return copy(
            N.at[:, t, at, :], o_ref.at[pl.ds(4 * gy, 4), at, :], osem.at[d], orem.at[d],
            {"gy": t},
        )

    def send_out(at):
        def one(d, _):
            out_window(d, at).start()
            return 0

        lax.fori_loop(1, ny, one, 0)
        pltpu.make_async_copy(
            N.at[:, gy, at, :], o_ref.at[pl.ds(4 * gy, 4), at, :], orem.at[0]
        ).start()

    def over(planes, work):
        def one(n, _):
            work(planes[0] + (planes[1] - planes[0]) * n)
            return 0

        lax.fori_loop(0, 2, one, 0)

    inner, outer = (2, 3), (1, 4)

    def half(c, planes, first=0, count=8):
        def plane(p):
            v = change_of(E, p, 8 * c + 9, F, 8 * c + 9)
            at = 8 * c + 8 + first if count < 8 else pl.multiple_of(8 * c + 8, 8)
            H[p, :, pl.ds(at, count), :] = v[:, first : first + count]

        over(planes, plane)

    def full(c, planes, first=0, count=8):
        def plane(p):
            v = change_of(H, p, 8 * c + 7, F, pl.multiple_of(8 * c + 8, 8))
            if count < 8:
                N[p - 1, :, pl.ds(8 * c + first, count), :] = v[:, first : first + count]
                row = lax.broadcasted_iota(jnp.int32, v.shape, 1)
                v = jnp.where((row >= first) & (row < first + count), v, 0.0)
            else:
                N[p - 1, :, pl.ds(pl.multiple_of(8 * c, 8), 8), :] = v
            acc[p - 1] += jnp.sum(v, axis=0)

        over(planes, plane)

    def wait_rows(kind, part, c):
        for d in range(nx):
            for x in x_rows(kind, d, part, c):
                x.wait() if d == 0 else x.wait_recv()

    def wait_tile(kind, c):
        wait_rows(kind, 1, c)

        @pl.when(c < tiles - 1)
        def _():
            wait_rows(kind, 0, lax.min(c + 1, tiles - 1))

    def wait_edges(side):
        @pl.when(has_edge(gx, side))
        def _():
            for d in range(nx):
                for x in x_edge(d, side):
                    x.wait() if d == 0 else x.wait_recv()

    def out_at(c):
        return pl.ds(pl.multiple_of(8 * c, 8), 8)

    def stage(d):
        t = lax.rem(gx + d, nx)
        return (
            pltpu.make_async_copy(e_ref.at[t * tiles], first_tile.at[0, t], fsem.at[0, d]),
            pltpu.make_async_copy(f_ref.at[3, t * tiles], first_tile.at[1, t], fsem.at[1, d]),
        )

    for d in range(1, nx):
        for x in stage(d):
            x.start()
    acc[...] = jnp.zeros_like(acc)
    for side, at, half_at in ((0, 7, 6), (1, 8 + rows, 7 + rows)):

        @pl.when(jnp.logical_not(has_edge(gx, side)))
        def _():
            none = jnp.zeros((4, ny, 1, 128), jnp.float32)
            E[1:5, :, at : at + 1, :] = none
            F[3, 1:5, :, at : at + 1, :] = none
            H[1:5, :, half_at : half_at + 1, :] = none

    pl.semaphore_wait(bar, nx + 1)
    for d in range(1, nx):
        for x in stage(d):
            x.wait()
    start_rows(0, 1, 0, True)
    start_rows(0, 0, 0, True)
    start_rows(0, 0, 1)
    start_edges(0)
    start_edges(1)
    start_rows(1, 0, 0)
    for c in range(1, AHEAD):
        start_tile(0, c)
        start_tile(1, c - 1)
    wait_edges(0)
    wait_rows(0, 0, 0)

    def greet(r):
        for n in (2**r, ring - 2**r):
            to = lax.rem(m + n, ring)
            pl.semaphore_signal(
                tok.at[r], inc=1, device_id={"gy": lax.rem(to, ny), "gz": to // ny},
                device_id_type=MESH,
            )

    def start_z(at, c):
        for way in (0, 1):
            for x in z_window(way, at, c):
                x.start()

    def wait_z(at, c):
        for way in (0, 1):
            for x in z_window(way, at, c):
                x.wait_recv()

    def start_h(at, c):
        for way in (0, 1):
            h_window(way, at, c).start()

    def wait_h(at, c):
        for way in (0, 1):
            h_window(way, at, c).wait_recv()

    def z_at(c):
        return pl.ds(8 * c + 9, 8)

    def h_at(c):
        return pl.ds(pl.multiple_of(8 * c + 8, 8), 8)

    z_first, h_first = pl.ds(8, 1), pl.ds(7, 1)
    last = tiles - 1
    h_last = pl.ds(8 * last + 8, 7)
    start_z(z_first, tiles)

    def step(c, _):
        @pl.when(c + AHEAD < tiles)
        def _():
            start_tile(0, c + AHEAD)

        @pl.when(c + AHEAD - 1 < tiles)
        def _():
            start_tile(1, c + AHEAD - 1)

        for r in range(rounds):

            @pl.when(c == r)
            def _():
                if r > 0:
                    pl.semaphore_wait(tok.at[r - 1], 2)
                greet(r)

        @pl.when(c == rounds)
        def _():
            pl.semaphore_wait(tok.at[rounds - 1], 2)

        @pl.when(c == last)
        def _():
            wait_edges(1)

        wait_tile(0, c)
        start_z(z_at(c), c)

        @pl.when(c == 1)
        def _():
            wait_rows(1, 0, 0)
            wait_z(z_first, tiles)
            half(-1, inner, 7, 1)
            half(-1, outer, 7, 1)
            start_h(h_first, tiles)

            @pl.when(has_edge(gx, 0))
            def _():
                x_half(0).start()

        @pl.when(c >= 1)
        def _():
            wait_tile(1, c - 1)
            half(c - 1, inner)
            wait_z(z_at(c - 1), c - 1)
            half(c - 1, outer)
            start_h(h_at(c - 1), c - 1)

        @pl.when(c == 2)
        def _():
            full(0, inner, 1, 7)
            wait_h(h_first, tiles)
            wait_h(h_at(0), 0)
            full(0, outer, 1, 7)

        @pl.when(c >= 3)
        def _():
            full(c - 2, inner)
            wait_h(h_at(c - 2), c - 2)
            full(c - 2, outer)

        @pl.when(c == 4)
        def _():
            send_out(pl.ds(1, 7))
            send_out(out_at(1))

        @pl.when(c >= 4)
        def _():
            send_out(out_at(c - 2))

        return 0

    lax.fori_loop(0, tiles, step, 0)
    wait_z(z_at(last), last)
    wait_rows(1, 1, last)
    half(last, outer, 0, 7)
    start_h(h_last, last)
    half(last, inner, 0, 7)

    @pl.when(has_edge(gx, 1))
    def _():
        x_half(1).start()

    full(last - 1, inner)
    wait_h(h_at(last - 1), last - 1)
    full(last - 1, outer)

    @pl.when(has_edge(gx, 1))
    def _():
        x_half(0).wait_recv()

    full(last, inner)
    wait_h(h_last, last)
    full(last, outer)

    @pl.when(has_edge(gx, 0))
    def _():
        x_half(1).wait_recv()
        H[1:5, :, 6:7, :] = below_row[...]

    full(0, inner, 0, 1)
    full(0, outer, 0, 1)

    lane = lax.broadcasted_iota(jnp.int32, (1, 128), 1)
    part = jnp.zeros((1, 128), jnp.float32)
    for p in range(4):
        part = part + jnp.where(
            lane == 4 * gy + p, jnp.sum(acc[p], axis=(0, 1), keepdims=True), 0.0
        )
    SM[0] = part
    SA[gx * ny + gy] = part

    def group_row(n):
        to = lax.rem(gx * ny + gy + n, nx * ny)
        return copy(
            SM.at[0], SA.at[gx * ny + gy], sa_s.at[n], sa_r.at[n],
            {"gx": to // ny, "gy": lax.rem(to, ny)},
        )

    def start_row(n, _):
        group_row(n).start()
        return 0

    def wait_row(n, _):
        group_row(n).wait()
        return 0

    lax.fori_loop(1, nx * ny, start_row, 0)
    send_out(out_at(last - 1))
    send_out(out_at(last))
    send_out(pl.ds(0, 1))
    lax.fori_loop(1, nx * ny, wait_row, 0)
    planes = jnp.sum(SA[...], axis=0)
    SM[1] = planes

    def lift(to_z, to_y, slot):
        return copy(
            SM.at[1], SC.at[gz], sc_s.at[to_z, slot], sc_r.at[gz], {"gy": to_y, "gz": to_z}
        )

    def lifts(act):
        for to in range(1, nz):
            alike = lax.rem(gz + to, 2) == 0

            @pl.when((gz < to) & alike)
            def _():
                act(lift(to, gy, 0))

            for end, first in ((ny - 1, 0), (1, ny // 2)):

                @pl.when((gz < to) & jnp.logical_not(alike) & (gy == end))
                def _():
                    for n in range(ny // 2):
                        act(lift(to, first + n, n))

    lifts(lambda x: x.start())
    for n in range(nz - 1):

        @pl.when(n < gz)
        def _():
            copy(SM.at[1], SC.at[n], sc_s.at[0, 0], sc_r.at[n], {"gz": gz}).wait_recv()

    below = jnp.zeros_like(planes)
    for n in range(nz - 1):
        below = below + jnp.where(n < gz, SC[n], 0.0)
    cells = 1.0 / (rows * nx * 128 * ny)
    mean = jnp.broadcast_to(planes * cells, (8, 128))
    lane = lax.broadcasted_iota(jnp.int32, (8, 128), 1)
    upto = mean
    for n in (1, 2, 4, 8, 16):
        upto = upto + jnp.where(lane >= n, pltpu.roll(upto, n, 1), 0.0)
    rank = (lane + (gz * 4 * ny + 1)).astype(jnp.float32)
    pm_ref[...] = mean
    rm_ref[...] = (upto + jnp.sum(below, axis=(0, 1), keepdims=True) * cells) / rank
    lifts(lambda x: x.wait_send())

    for d in range(ny):
        whole = o_ref.at[pl.ds(0, 4)]
        if d == 0:
            pltpu.make_async_copy(N.at[:, 0, pl.ds(0, rows), :], whole, orem.at[0]).wait()
        else:
            end = copy(
                N.at[:, 0, pl.ds(0, rows), :], whole, osem.at[d], orem.at[d],
                {"gy": lax.rem(gy + d, ny)},
            )
            end.wait()
    for d in range(1, nx):
        to = {"gx": lax.rem(gx + d, nx)}
        at = pl.ds(8, rows)
        copy(E.at[1, :, at, :], E.at[1, :, at, :], xsE.at[d], xrE.at[0, d, 0], to).wait_send()
        copy(E.at[1, :, at, :], E.at[1, :, at, :], xsK.at[d], xrK.at[0, d, 0], to).wait_send()
        three = F.at[pl.ds(0, 3), 1, :, at, :]
        copy(three, three, xsU.at[d], xrU.at[0, d, 0], to).wait_send()
        for side in (0, 1):

            @pl.when(has_edge(lax.rem(gx + d, nx), side))
            def _():
                for x in x_edge(d, side):
                    x.wait_send()
    for side in (0, 1):

        @pl.when(has_edge(gx, side))
        def _():
            x_half(side).wait_send()

    for way in (0, 1):
        for x in z_window(way, pl.ds(8, rows + 1), 0):
            x.wait_send()
        h_window(way, pl.ds(7, rows), 0).wait_send()


def per_device(energy, flow):
    nx, ny, nz = (lax.axis_size(a) for a in ("gx", "gy", "gz"))
    e = energy.reshape(32, 8, 8, 128).transpose(0, 2, 1, 3)
    f = flow.reshape(4, 32, 8, 8, 128).transpose(0, 1, 3, 2, 4)
    vmem = pl.BlockSpec(memory_space=pltpu.VMEM)
    hbm = pl.BlockSpec(memory_space=pl.ANY)
    f32 = jnp.float32
    dma = pltpu.SemaphoreType.DMA
    result, mean, running = pl.pallas_call(
        functools.partial(kernel, nx, ny, nz),
        out_shape=(
            jax.ShapeDtypeStruct((32, 64, 128), f32),
            jax.ShapeDtypeStruct((8, 128), f32),
            jax.ShapeDtypeStruct((8, 128), f32),
        ),
        in_specs=[hbm, hbm],
        out_specs=(hbm, vmem, vmem),
        scratch_shapes=[
            pltpu.VMEM((6, 8, 80, 128), f32),
            pltpu.VMEM((4, 6, 8, 80, 128), f32),
            pltpu.VMEM((6, 8, 80, 128), f32),
            pltpu.VMEM((4, 8, 64, 128), f32),
            pltpu.VMEM((4, 8, 1, 128), f32),
            pltpu.VMEM((2, 4, 8, 8, 128), f32),
            pltpu.VMEM((4, 8, 128), f32),
            pltpu.VMEM((32, 1, 128), f32),
            pltpu.VMEM((8, 1, 128), f32),
            pltpu.VMEM((2, 1, 128), f32),
            dma((4,)), dma((4,)), dma((4,)), dma((2, 4, 8)), dma((2, 4, 8)), dma((2, 4, 8)),
            dma((4, 2)), dma((4, 2)), dma((4, 2)), dma((4, 2)), dma((2,)), dma((2,)),
            dma((2,)), dma((2,)), dma((2,)), dma((2, 9)), dma((2, 9)), dma((2, 9)),
            dma((8,)), dma((8,)), dma((2, 4)),
            dma((32,)), dma((32,)), dma((8, 4)), dma((8,)),
            pltpu.SemaphoreType.REGULAR((8,)),
        ],
        compiler_params=pltpu.CompilerParams(
            collective_id=0, has_side_effects=True, vmem_limit_bytes=55_000_000
        ),
        name="two_steps",
    )(e, f)
    return result, mean[0, :32], running[0, :32]


def solution(mesh):
    placed = (P(("gz", "gy", "gx"), None, None), P(None, ("gz", "gy", "gx"), None, None))
    return jax.shard_map(
        per_device,
        mesh=mesh,
        in_specs=placed,
        out_specs=(P("gz", "gx", "gy"), P("gz"), P("gz")),
        check_vma=False,
    )
```
